256 devices in a mesh: dp: 8 (over z_hi, core), comp: 32 (over x, z_lo, y).
Axes of the slice: x: 4, y: 4, z: 8 (z_hi: 4, z_lo: 2; z = z_hi * 2 + z_lo), core: 2. Of those that a mesh axis runs over, the one named last changes fastest.
Arguments:
- row_ids: int32 [8192], P('dp'), may hold values from 0 to 8191
- table: float32 [8192, 1024], P('comp'), may hold values from -25 to 25, as said below
- means: float32 [16384, 1024], P('comp'), may hold values from -0.3 to 0.3
- precisions: float32 [16384, 1024], P('comp'), may hold values from 0.8 to 1.2
- mix_logits: float32 [16384], P('comp'), may hold values from -2 to 2
- step_index: int32 [1], replicated, may hold values from 0 to 65535
Outputs:
- new_means: float32 [16384, 1024], P('comp')
- new_precisions: float32 [16384, 1024], P('comp')
- new_logits: float32 [16384], P('comp')
The draws below stay inside these ranges and needn't reach their ends.
Inputs may be any that keep to these rules, and one draw needn't show every extreme that they name: `table`: embedding rows with entries of order one and row scales that differ.
All inputs are finite; a program needn't handle non-finite values.
Results may differ from the reference program's by a relative error of at most 0.0014.
Values sent between devices are 32-bit elements; how exact they have to be, the bound alone decides.
A program may use at most 64 MiB of HBM per device.

```python
import jax
import jax.numpy as jnp
from jax import lax

D = 1024
ROWS = 1024
K = 16384
BATCH = 8192
TABLE = 8192
N_DP = 8


def draw_table(key, part):
    key_base = jax.random.fold_in(key, 11)
    key_rows = jax.random.fold_in(key, 12)
    key_cols = jax.random.fold_in(key, 13)
    base = jnp.clip(jax.random.normal(key_base, (TABLE, D), jnp.float32), -5.0, 5.0)
    row_scale = jnp.exp(jax.random.uniform(key_rows, (TABLE, 1), jnp.float32, -0.7, 0.7))
    col_scale = jnp.exp(jax.random.uniform(key_cols, (1, D), jnp.float32, -0.35, 0.35))
    return (base * row_scale * col_scale).astype(jnp.float32)


def plant(result, own_key, low, top_value):
    dims = result.shape
    spot = [jax.random.randint(jax.random.fold_in(own_key, axis), (), 0, dims[axis]) for axis in range(len(dims))]
    result = result.at[tuple(spot)].set(low)
    longest = dims.index(max(dims))
    spot[longest] = (spot[longest] + 1) % dims[longest]
    return result.at[tuple(spot)].set(top_value)


def block_scale(rng, extent, split, smallest, high):
    factor_of, own = 1.0, jax.random.fold_in(rng, 6)
    for dim, blocks in split:
        draws = jnp.exp(jax.random.uniform(jax.random.fold_in(own, dim), (blocks,), jnp.float32, smallest / len(split), high / len(split)))
        factor_of = factor_of * jnp.repeat(draws, extent[dim] // blocks).reshape([-1 if axis == dim else 1 for axis in range(len(extent))])
    return factor_of


def centred(key, extent, scale, reach, pieces=(), held_as=jnp.bfloat16):
    entries = jax.random.normal(key, extent, jnp.float32) * scale
    if len(pieces) > 0:
        entries = block_scale(key, extent, pieces, -0.22, 0.18) * entries
    return jnp.clip(entries, min=-reach, max=reach).astype(held_as)


def setup_inputs(seed: int = 0) -> dict:
    arg_keys = jax.random.split(jax.random.key(seed), 7)
    row_ids = plant(jax.random.randint(arg_keys[0], (BATCH,), 0, TABLE), jax.random.fold_in(arg_keys[0], 1), 0, TABLE - 1).astype(jnp.int32)
    table = draw_table(jax.random.fold_in(arg_keys[6], 71), 0)
    means = centred(arg_keys[2], (K, D), 0.05, 0.3, ((0, 32),), jnp.float32)
    precisions = jnp.clip(1.0 + 0.04 * jax.random.normal(arg_keys[3], (K, D), jnp.float32), 0.8, 1.2)
    mix_logits = jnp.clip(jax.random.uniform(arg_keys[4], (K,), jnp.float32, -2.0, 2.0) * block_scale(arg_keys[4], (K,), ((0, 32),), -0.4, 0.0), -2.0, 2.0)
    step_index = jax.random.randint(arg_keys[5], (1,), 0, 65536).astype(jnp.int32)
    return dict(row_ids=row_ids, table=table, means=means, precisions=precisions, mix_logits=mix_logits, step_index=step_index)


def update(weights, means, precisions, counts, first_moment, second_moment, step_size, batch):
    retain = 1.0 - step_size
    mass_new = retain * weights + step_size * counts / batch
    prior = (retain * weights)[:, None]
    new_means = (prior * means + step_size * first_moment / batch) / mass_new[:, None]
    moved = means - new_means
    spread = prior * (1.0 / precisions + moved * moved) + step_size * (second_moment - 2.0 * new_means * first_moment + new_means * new_means * counts[:, None]) / batch
    return new_means, mass_new[:, None] / spread, jnp.log(mass_new)


def reference(row_ids, table, means, precisions, mix_logits, step_index):
    highest = lax.Precision.HIGHEST
    samples = jnp.take(table, row_ids, axis=0)
    logit_top = jnp.max(mix_logits)
    raised = jnp.exp(mix_logits - logit_top)
    weights = raised / jnp.sum(raised)
    stacked = jnp.concatenate([precisions, -2.0 * precisions * means], axis=1)
    offset = mix_logits + 0.5 * jnp.sum(jnp.log(precisions), axis=1) - 0.5 * jnp.sum(precisions * means * means, axis=1)

    def group_step(totals, block_rows):
        squares = block_rows * block_rows
        features = jnp.concatenate([squares, block_rows], axis=1)
        quadratic = jnp.dot(features, stacked.T, precision=highest, preferred_element_type=jnp.float32)
        scores = offset[None, :] - 0.5 * quadratic
        peak_rows = jnp.max(scores, axis=1, keepdims=True)
        raised_rows = jnp.exp(scores - peak_rows)
        resp = raised_rows / jnp.sum(raised_rows, axis=1, keepdims=True)
        counts = totals[0] + jnp.sum(resp, axis=0)
        first_moment = totals[1] + jnp.dot(resp.T, block_rows, precision=highest, preferred_element_type=jnp.float32)
        second_moment = totals[2] + jnp.dot(resp.T, squares, precision=highest, preferred_element_type=jnp.float32)
        return (counts, first_moment, second_moment), None

    start_totals = (jnp.zeros((K,), jnp.float32), jnp.zeros((K, D), jnp.float32), jnp.zeros((K, D), jnp.float32))
    totals, unused = lax.scan(group_step, start_totals, samples.reshape(N_DP, ROWS, D))
    step_size = (2.0 + step_index[0].astype(jnp.float32) / 8192.0) ** -0.6
    new_means, new_precisions, new_logits = update(weights, means, precisions, totals[0], totals[1], totals[2], step_size, 1.0 * BATCH)
    return new_means, new_precisions, new_logits
```

```python
import jax
import jax.numpy as jnp
from jax import lax
from jax.sharding import PartitionSpec as P


def split(value):
    high = lax.reduce_precision(value, 8, 7)
    return high.astype(jnp.bfloat16), (value - high).astype(jnp.bfloat16)


def product(left, right, dims):
    def one(a, b):
        return lax.dot_general(a, b, (dims, ((), ())), preferred_element_type=jnp.float32)

    return one(left[0], right[0]) + (one(left[0], right[1]) + one(left[1], right[0]))


def multiplicity(ids, part, parts, owners, share):
    per_owner = parts * share
    owner = ids // per_owner
    within = ids % per_owner
    mine = (within // share) == part
    row = within % share
    left = (owner[None, :] == lax.broadcasted_iota(jnp.int32, (owners, 1), 0)) & mine[None, :]
    right = row[None, :] == lax.broadcasted_iota(jnp.int32, (share, 1), 0)
    found = lax.dot_general(
        left.astype(jnp.bfloat16),
        right.astype(jnp.bfloat16),
        (((1,), (1,)), ((), ())),
        preferred_element_type=jnp.float32,
    )
    return found.reshape(-1)


def local(row_ids, table, means, precisions, mix_logits, step_index):
    dp, comp = lax.axis_size("dp"), lax.axis_size("comp")
    part = lax.axis_index("dp")
    share = table.shape[0] // dp
    batch = 1.0 * row_ids.shape[0] * dp
    ids = lax.all_gather(row_ids, "dp", tiled=True)
    mine = lax.dynamic_slice_in_dim(table, part * share, share, 0)
    samples = lax.all_gather(mine, "comp", tiled=True)
    times = multiplicity(ids, part, dp, comp, share)

    squares = samples * samples
    s, q = split(samples), split(squares)
    excess = precisions - 1.0
    cross = -2.0 * precisions * means
    e, c = split(excess), split(cross)
    offset = (
        mix_logits
        + 0.5 * jnp.sum(jnp.log(precisions), axis=1)
        - 0.5 * jnp.sum(precisions * means * means, axis=1)
    )
    lanes = ((1,), (1,))
    quadratic = product(e, q, lanes) + product(c, s, lanes)
    scores = offset[:, None] - 0.5 * quadratic
    top = jnp.max(scores, axis=0)
    raised = jnp.exp(scores - top[None, :])
    mass = jnp.sum(raised, axis=0)
    logit_top = jnp.max(mix_logits)
    logit_raised = jnp.exp(mix_logits - logit_top)
    logit_mass = jnp.sum(logit_raised)
    packed = jnp.concatenate([top, mass, jnp.full((128,), logit_top), jnp.full((128,), logit_mass)])
    every = lax.all_gather(packed, "comp")
    rows = top.shape[0]
    tops, masses = every[:, :rows], every[:, rows : 2 * rows]
    peak = jnp.max(tops, axis=0)
    total = jnp.sum(masses * jnp.exp(tops - peak[None, :]), axis=0)
    factor = jnp.exp(top - peak) / total * times
    resp = raised * factor[None, :]
    logit_tops, logit_masses = every[:, 2 * rows], every[:, 2 * rows + 128]
    logit_peak = jnp.max(logit_tops)
    logit_total = jnp.sum(logit_masses * jnp.exp(logit_tops - logit_peak))
    weights = logit_raised * (jnp.exp(logit_top - logit_peak) / logit_total)

    counts = jnp.sum(resp, axis=1)
    r = split(resp)
    inner = ((1,), (0,))
    first = product(r, s, inner)
    second = product(r, q, inner)
    first, second = (lax.psum_scatter(x, "dp", scatter_dimension=0, tiled=True) for x in (first, second))
    counts = lax.psum(counts, "dp")

    def own(x):
        size = x.shape[0] // dp
        return lax.dynamic_slice_in_dim(x, part * size, size, 0)

    step = (2.0 + step_index[0].astype(jnp.float32) / 8192.0) ** (-0.6)
    retain = 1.0 - step
    mass_all = retain * weights + step * counts / batch
    new_logits = jnp.log(mass_all)
    mass_new = own(mass_all)[:, None]
    prior = own(retain * weights)[:, None]
    own_counts = own(counts)[:, None]
    own_means = own(means)
    new_means = (prior * own_means + step * first / batch) / mass_new
    moved = own_means - new_means
    spread = (
        prior * (1.0 / own(precisions) + moved * moved)
        + step * (second - 2.0 * new_means * first + new_means * new_means * own_counts) / batch
    )
    new_precisions = mass_new / spread
    new_means, new_precisions = (lax.all_gather(x, "dp", tiled=True) for x in (new_means, new_precisions))
    return new_means, new_precisions, new_logits


def solution(mesh):
    placed = (P("dp"), P("comp", None), P("comp", None), P("comp", None), P("comp"), P())
    return jax.shard_map(
        local,
        mesh=mesh,
        in_specs=placed,
        out_specs=(P("comp", None), P("comp", None), P("comp")),
        check_vma=False,
    )
```

```python
import functools

import jax
import jax.numpy as jnp
from jax import lax
from jax.experimental import pallas as pl
from jax.experimental.pallas import tpu as pltpu
from jax.sharding import PartitionSpec as P

F32, BF16 = jnp.float32, jnp.bfloat16
NX, NZ, NY = 4, 2, 4
NH, NC = 4, 2
LANES = (((1,), (1,)), ((), ()))
INNER = (((1,), (0,)), ((), ()))


def split(value):
    high = value.astype(BF16)
    return high, (value - high.astype(F32)).astype(BF16)


def mul(left, right, dims, precision=None):
    return lax.dot_general(left, right, dims, precision=precision, preferred_element_type=F32)


class Copy:
    def __init__(self, src, dst, send_sem, recv_sem, to):
        self.make = lambda: pltpu.make_async_remote_copy(
            src_ref=src, dst_ref=dst, send_sem=send_sem, recv_sem=recv_sem, device_id={"dp": to}
        )

    def start(self):
        self.make().start()

    def wait_send(self):
        self.make().wait_send()

    def wait_recv(self):
        self.make().wait_recv()


def kernel(
    ids_ref, table_ref, means_ref, prec_ref, logits_ref, step_ref,
    out_m, out_p, out_l,
    rows, ids_all, a_hi, a_lo, f_hi, f_lo, score, r_hi, r_lo, offset, tops, times_ref,
    xb, yb, zb, counts_all, columns,
    sib_out, sib_in, part, from_r, from_l, own_r, own_l,
    local_sem, ids_send, ids_recv, row_send, row_recv, xs, xr, ys, yr, zs, zr, cs, cr,
    sib_s, sib_r, opp_s, opp_r, dir_s, dir_r, acc_s, acc_r,
    gz_s, gz_r, gf_s, gs_s, gs_r,
):
    dp, comp = lax.axis_index("dp"), lax.axis_index("comp")
    h, core = dp // NC, dp % NC
    x, zl, y = comp // (NZ * NY), (comp // NY) % NZ, comp % NY
    n_dp = NH * NC
    share = rows.shape[1]
    half = share // 2
    comps, width = means_ref.shape
    n_rows = f_hi.shape[0]

    def at(dx, dz, dy):
        return ((x + dx) % NX) * (NZ * NY) + ((zl + dz) % NZ) * NY + (y + dy) % NY

    def dp_at(dh, dc):
        return ((h + dh) % NH) * NC + (core + dc) % NC

    peers_c = [at(d, 0, 0) for d in (1, 2, 3)] + [at(0, 0, d) for d in (1, 2, 3)] + [at(0, 1, 0)]
    peers_d = [dp_at(a, b) for a in range(NH) for b in range(NC) if (a, b) != (0, 0)]
    barrier = pltpu.get_barrier_semaphore()
    for peer in peers_c:
        pl.semaphore_signal(barrier, inc=1, device_id={"comp": peer})
    for peer in peers_d:
        pl.semaphore_signal(barrier, inc=1, device_id={"dp": peer})
    pl.semaphore_wait(barrier, len(peers_c) + len(peers_d))

    waits = []

    def send(src, dst, send_sem, recv_sem, **where):
        copy = pltpu.make_async_remote_copy(
            src_ref=src, dst_ref=dst, send_sem=send_sem, recv_sem=recv_sem, device_id=where
        )
        copy.start()
        return copy

    me = at(0, 0, 0)
    mine = pltpu.make_async_copy(table_ref.at[pl.ds(dp * share, share)], rows.at[me], local_sem.at[0])
    mine.start()
    sends = [0]

    def piece(ref, slot, b):
        return ref.at[slot, pl.ds(b * half, half)]

    def push(slot, b, dx, dz, dy, source=None):
        src = piece(rows, slot, b) if source is None else source
        k = sends[0]
        sends[0] += 1
        waits.append(
            send(src, piece(rows, slot, b), row_send.at[k], row_recv.at[slot, b], comp=at(dx, dz, dy))
        )

    def arrived(slot, b):
        pltpu.make_async_copy(piece(rows, slot, b), piece(rows, slot, b), row_recv.at[slot, b]).wait()

    def own(b):
        return table_ref.at[pl.ds(dp * share + b * half, half)]

    for b in (0, 1):
        push(me, b, 0, 1, 0, own(b))
    first = [(1, 0, 0), (-1, 0, 0)], [(0, 0, 1), (0, 0, -1)]
    for b in (0, 1):
        for to in first[b]:
            push(me, b, *to, own(b))
    for b in (0, 1):
        for to in first[1 - b]:
            push(me, b, *to, own(b))
    ids_copies = [
        send(ids_ref, ids_all.at[dp], ids_send.at[k], ids_recv.at[dp], dp=peer)
        for k, peer in enumerate(peers_d)
    ]
    ids_all[dp] = ids_ref[...]

    row_block = 32

    def factors(i, carry):
        at_rows = pl.ds(pl.multiple_of(i * row_block, row_block), row_block)
        p, m = prec_ref[at_rows, :], means_ref[at_rows, :]
        cross = p * m
        hi, lo = split(cross)
        a_hi[at_rows, :width], a_lo[at_rows, :width] = hi, lo
        hi, lo = split(-0.5 * (p - 1.0))
        a_hi[at_rows, width:], a_lo[at_rows, width:] = hi, lo
        offset[at_rows, :] = 0.5 * jnp.sum(jnp.log(p) - cross * m, axis=1, keepdims=True)
        return carry

    for b in (0, 1):
        arrived(at(0, 1, 0), b)
        for to in first[b] + first[1 - b]:
            push(at(0, 1, 0), b, *to)
    lax.fori_loop(0, comps // row_block, factors, 0)
    logits = logits_ref[...]
    turned = jnp.transpose(jnp.broadcast_to(logits, (8, comps)))
    offset[...] = offset[...] + turned[:, 0:1]

    def vec(d, b):
        return (d, 0) if b == 0 else (0, d)

    for rel in (0, 1):
        for b in (0, 1):
            for d in (-1, 1):
                dx, dy = vec(d, b)
                slot = at(dx, rel, dy)
                arrived(slot, b)
                if (rel == 0) == (d == -1):
                    fx, fy = vec(-d, b)
                    push(slot, b, fx, 0, fy)
                for to in first[1 - b]:
                    push(slot, b, *to)
    for rel in (0, 1):
        for b in (0, 1):
            dx, dy = vec(2, b)
            slot = at(dx, rel, dy)
            arrived(slot, b)
            for to in first[1 - b]:
                push(slot, b, *to)
    for e in (0, -1, 1, 2):
        for rel in (0, 1):
            for b in (0, 1):
                ex, ey = vec(e, b)
                for d in (-1, 1):
                    dx, dy = vec(d, 1 - b)
                    slot = at(ex + dx, rel, ey + dy)
                    arrived(slot, b)
                    if (rel == 0) == (d == -1):
                        fx, fy = vec(-d, 1 - b)
                        push(slot, b, fx, 0, fy)
    for e in (0, -1, 1, 2):
        for rel in (0, 1):
            for b in (0, 1):
                ex, ey = vec(e, b)
                dx, dy = vec(2, 1 - b)
                arrived(at(ex + dx, rel, ey + dy), b)
    mine.wait()

    found = jnp.zeros((NX * NZ * NY, share), F32)
    for k, peer in enumerate(peers_d):
        pltpu.make_async_copy(ids_ref, ids_all.at[peer], ids_recv.at[peer]).wait()
    per_owner = n_dp * share
    for k in range(n_dp):
        ids = ids_all[k]
        owner = ids // per_owner
        within = ids - owner * per_owner
        row = within - dp * share
        left = lax.broadcasted_iota(jnp.int32, (NX * NZ * NY, ids.shape[1]), 0) == owner
        right = lax.broadcasted_iota(jnp.int32, (share, ids.shape[1]), 0) == row
        found += mul(left.astype(F32).astype(BF16), right.astype(F32).astype(BF16), LANES)
    flat = lax.broadcasted_iota(jnp.int32, (NX * NZ * NY, n_rows), 1)
    slot_of = lax.broadcasted_iota(jnp.int32, (NX * NZ * NY, n_rows), 0)
    pick = (flat // share == slot_of).astype(F32)
    spread_out = mul(found, pick, (((0,), (0,)), ((), ())), lax.Precision.HIGHEST)
    row_of = lax.broadcasted_iota(jnp.int32, (share, n_rows), 0)
    row_flat = lax.broadcasted_iota(jnp.int32, (share, n_rows), 1)
    times_ref[...] = jnp.sum(jnp.where(row_flat % share == row_of, spread_out, 0.0), axis=0, keepdims=True)

    per = NZ * NY
    chunk = per * share
    tile = 256

    def features(slot, carry):
        s = rows[slot]
        here = pl.ds(pl.multiple_of(slot * share, share), share)
        f_hi[here, :width], f_lo[here, :width] = split(s)
        f_hi[here, width:], f_lo[here, width:] = split(s * s)
        return carry

    def plane(c):
        lax.fori_loop(c * per, (c + 1) * per, features, 0)
        cols = pl.ds(pl.multiple_of(c * chunk, chunk), chunk)

        def block(k, top):
            here = pl.ds(pl.multiple_of(k * tile, tile), tile)
            fh, fl = f_hi[cols, :], f_lo[cols, :]
            s = mul(a_hi[here, :], fh, LANES) + mul(a_hi[here, :], fl, LANES) + mul(a_lo[here, :], fh, LANES)
            s = s + offset[here, :]
            score[here, cols] = s
            return jnp.maximum(top, jnp.max(s, axis=0, keepdims=True))

        top = lax.fori_loop(0, comps // tile, block, jnp.full((1, chunk), -jnp.inf, F32))

        def raise_block(k, mass):
            here = pl.ds(pl.multiple_of(k * 64, 64), 64)
            e = jnp.exp(score[here, cols] - top)
            score[here, cols] = e
            return mass + jnp.sum(e, axis=0, keepdims=True)

        mass = lax.fori_loop(0, comps // 64, raise_block, jnp.zeros((1, chunk), F32))
        tops[:, cols] = top
        xb[x, :, cols] = top
        xb[x, :, pl.ds(pl.multiple_of(n_rows + c * chunk, chunk), chunk)] = mass

    for d in (0, -1, 1, 2):
        plane((x + d) % NX)

    logit_top = jnp.max(logits)
    logit_raised = jnp.exp(logits - logit_top)
    xb[x, :, pl.ds(2 * n_rows, 128)] = jnp.full((1, 128), logit_top, F32)
    xb[x, :, pl.ds(2 * n_rows + 128, 128)] = jnp.full((1, 128), jnp.sum(logit_raised), F32)

    def combine(ref, n):
        out = []
        for start, size in ((0, n_rows), (2 * n_rows, 128)):
            gap = n_rows if start == 0 else 128
            ts = [ref[k, :, start : start + size] for k in range(n)]
            ms = [ref[k, :, start + gap : start + gap + size] for k in range(n)]
            t = functools.reduce(jnp.maximum, ts)
            out.append((start, size, gap, t, sum(m * jnp.exp(a - t) for m, a in zip(ms, ts))))
        return out

    def fill(ref, index, results):
        for start, size, gap, t, m in results:
            ref[index, :, start : start + size] = t
            ref[index, :, start + gap : start + gap + size] = m

    def exchange(ref, index, peers, slots, s_sem, r_sem):
        copies = [
            send(ref.at[index], ref.at[index], s_sem.at[k], r_sem.at[index], comp=peer)
            for k, peer in enumerate(peers)
        ]
        for slot in slots:
            pltpu.make_async_copy(ref.at[slot], ref.at[slot], r_sem.at[slot]).wait()
        for copy in copies:
            copy.wait_send()

    exchange(xb, x, [at(d, 0, 0) for d in (1, 2, 3)], [(x + d) % NX for d in (1, 2, 3)], xs, xr)
    fill(yb, y, combine(xb, NX))
    exchange(yb, y, [at(0, 0, d) for d in (1, 2, 3)], [(y + d) % NY for d in (1, 2, 3)], ys, yr)
    fill(zb, zl, combine(yb, NY))
    exchange(zb, zl, [at(0, 1, 0)], [(zl + 1) % NZ], zs, zr)
    (_, _, _, peak, total), (_, _, _, logit_peak, logit_total) = combine(zb, NZ)
    factor = jnp.exp(tops[...] - peak) / total * times_ref[...]

    def responsibilities(k, carry):
        here = pl.ds(pl.multiple_of(k * row_block, row_block), row_block)
        r_hi[here, :], r_lo[here, :] = split(score[here, :] * factor)
        return carry

    lax.fori_loop(0, comps // row_block, responsibilities, 0)
    ones = jnp.ones((8, n_rows), BF16)
    mass_k = mul(ones, r_hi[...], LANES) + mul(ones, r_lo[...], LANES)
    counts_all[dp] = mass_k[0:1, :]
    count_copies = [
        send(counts_all.at[dp], counts_all.at[dp], cs.at[k], cr.at[dp], dp=peer)
        for k, peer in enumerate(peers_d)
    ]

    n_blocks = 2 * width // tile
    own_half = comps // NC
    q = own_half // NH
    side = tile // 2
    L, R = dp_at(-1, 0), dp_at(1, 0)
    sib = dp_at(0, 1)

    def moment(n, which):
        start = pl.multiple_of((n % 2) * width + (n // 2) * tile, tile)
        cols = pl.ds(start, tile)
        here = pl.ds(pl.multiple_of(which * own_half, own_half), own_half)
        fh, fl, rh = f_hi[:, cols], f_lo[:, cols], r_hi[here, :]
        return mul(rh, fh, INNER) + mul(rh, fl, INNER) + mul(r_lo[here, :], fh, INNER)

    def sib_copy(n):
        return pltpu.make_async_remote_copy(
            src_ref=sib_out.at[n], dst_ref=sib_in.at[n], send_sem=sib_s.at[n], recv_sem=sib_r.at[n],
            device_id={"dp": sib},
        )

    def for_sibling(n):
        sib_out[n] = moment(n, 1 - core)
        sib_copy(n).start()

    def chunk_of(n, o, b):
        return part.at[n, pl.ds(pl.multiple_of(o * q, q), q), pl.ds(b * side, side)]

    left_h, right_h, far_h = (h - 1) % NH, (h + 1) % NH, (h + 2) % NH

    def remote(src, dst, s, r, to):
        return Copy(src, dst, s, r, to)

    def cols_of(b):
        return pl.ds(b * side, side)

    def z_copies(n):
        return [
            remote(chunk_of(n, far_h, 0), from_r.at[n], opp_s.at[n, 0], opp_r.at[n, 0], L),
            remote(chunk_of(n, far_h, 1), from_l.at[n], opp_s.at[n, 1], opp_r.at[n, 1], R),
            remote(chunk_of(n, left_h, 1), own_r.at[n, :, cols_of(1)], dir_s.at[n, 0], dir_r.at[n, 0], L),
            remote(chunk_of(n, right_h, 0), own_l.at[n, :, cols_of(0)], dir_s.at[n, 1], dir_r.at[n, 1], R),
        ]

    def acc_copies(n):
        return [
            remote(chunk_of(n, left_h, 0), own_r.at[n, :, cols_of(0)], acc_s.at[n, 0], acc_r.at[n, 0], L),
            remote(chunk_of(n, right_h, 1), own_l.at[n, :, cols_of(1)], acc_s.at[n, 1], acc_r.at[n, 1], R),
        ]

    def relay(n):
        opp, acc = z_copies(n)[:2], acc_copies(n)
        opp[0].wait_recv()
        spot = chunk_of(n, left_h, 0)
        spot[...] = spot[...] + from_r[n]
        acc[0].start()
        opp[1].wait_recv()
        spot = chunk_of(n, right_h, 1)
        spot[...] = spot[...] + from_l[n]
        acc[1].start()

    for_sibling(0)

    def reduce_step(n, carry):
        @pl.when(n + 1 < n_blocks)
        def _():
            for_sibling(n + 1)

        own_block = moment(n, core)
        sib_copy(n).wait_recv()
        part[n] = own_block + sib_in[n]
        for copy in z_copies(n):
            copy.start()

        @pl.when(n > 0)
        def _():
            relay(n - 1)

        return carry

    lax.fori_loop(0, n_blocks, reduce_step, 0)
    relay(n_blocks - 1)

    for k, peer in enumerate(peers_d):
        pltpu.make_async_copy(counts_all.at[peer], counts_all.at[peer], cr.at[peer]).wait()
    counts = sum(counts_all[k] for k in range(n_dp))
    batch = 1.0 * n_dp * ids_ref.shape[1]
    index = jnp.full((1, comps), step_ref[0].astype(F32), F32)
    step = jnp.exp(-0.6 * jnp.log(2.0 + index / 8192.0))
    retain = 1.0 - step
    weights = logit_raised * (jnp.exp(logit_top - logit_peak[:, 0:1]) / logit_total[:, 0:1])
    prior = retain * weights
    mass_new = prior + step * counts / batch
    out_l[...] = jnp.log(mass_new)
    stacked = jnp.concatenate([mass_new, prior, counts, step, mass_new, prior, counts, step], axis=0)
    columns[...] = jnp.transpose(stacked)

    mine_at = pl.ds(pl.multiple_of(core * own_half + h * q, q), q)
    col = columns[mine_at, :]
    mass_c, prior_c, counts_c, step_c = (col[:, k : k + 1] for k in range(4))

    def reduced(n):
        z, acc = z_copies(n), acc_copies(n)
        for copy in (z[2], z[3], acc[0], acc[1]):
            copy.wait_recv()
        return part[n, pl.ds(pl.multiple_of(h * q, q), q), :] + own_r[n] + own_l[n]

    outs = (out_m, out_p)

    def out_piece(a, cb, o, c):
        here = pl.ds(pl.multiple_of(c * own_half + o * q, q), q)
        return outs[a].at[here, pl.ds(pl.multiple_of(cb * tile, tile), tile)]

    def z_gather(a, cb, o, s, r, to):
        return remote(out_piece(a, cb, o, core), out_piece(a, cb, o, core), s, r, to)

    def own_sends(cb):
        found = []
        for a in (0, 1):
            found.append(z_gather(a, cb, h, gz_s.at[cb, a, 0], gz_r.at[cb, a, 0], R))
            found.append(z_gather(a, cb, h, gz_s.at[cb, a, 1], gz_r.at[cb, a, 1], L))
            found.append(z_gather(a, cb, h, gs_s.at[cb, a, 0], gs_r.at[cb, a, 0], sib))
        return found

    def forwards(cb):
        return [
            z_gather(0, cb, left_h, gf_s.at[cb, 0], gz_r.at[cb, 0, 2], R),
            z_gather(1, cb, right_h, gf_s.at[cb, 1], gz_r.at[cb, 1, 2], L),
        ]

    def sib_sends(cb, a, k):
        o = (left_h, right_h, far_h)[k]
        return z_gather(a, cb, o, gs_s.at[cb, a, 1 + k], gs_r.at[cb, a, 1 + k], sib)

    def z_arrived(cb, a, k):
        o = (left_h, right_h, far_h)[k]
        ref = out_piece(a, cb, o, core)
        pltpu.make_async_copy(ref, ref, gz_r.at[cb, a, k]).wait()

    def update(cb, carry):
        first_m, second_m = reduced(2 * cb), reduced(2 * cb + 1)
        cols = pl.ds(pl.multiple_of(cb * tile, tile), tile)
        m, p = means_ref[mine_at, cols], prec_ref[mine_at, cols]
        new_m = (prior_c * m + step_c * first_m / batch) / mass_c
        moved = m - new_m
        spread = (
            prior_c * (1.0 / p + moved * moved)
            + step_c * (second_m - 2.0 * new_m * first_m + new_m * new_m * counts_c) / batch
        )
        out_m[mine_at, cols] = new_m
        out_p[mine_at, cols] = mass_c / spread
        for copy in own_sends(cb):
            copy.start()

        @pl.when(cb > 0)
        def _():
            pass_on(cb - 1)

        return carry

    def pass_on(cb):
        fwd = forwards(cb)
        z_arrived(cb, 0, 0)
        fwd[0].start()
        z_arrived(cb, 1, 1)
        fwd[1].start()
        sib_sends(cb, 0, 0).start()
        sib_sends(cb, 1, 1).start()
        z_arrived(cb, 1, 0)
        sib_sends(cb, 1, 0).start()
        z_arrived(cb, 0, 1)
        sib_sends(cb, 0, 1).start()

    n_cols = width // tile
    lax.fori_loop(0, n_cols, update, 0)
    pass_on(n_cols - 1)

    def finish(cb, carry):
        for a in (0, 1):
            z_arrived(cb, a, 2)
            sib_sends(cb, a, 2).start()
        return carry

    lax.fori_loop(0, n_cols, finish, 0)

    def drain(cb, carry):
        for copy in own_sends(cb) + forwards(cb):
            copy.wait_send()
        for a in (0, 1):
            for k in range(3):
                sib_sends(cb, a, k).wait_send()
            for k, o in enumerate((h, left_h, right_h, far_h)):
                ref = out_piece(a, cb, o, 1 - core)
                pltpu.make_async_copy(ref, ref, gs_r.at[cb, a, k]).wait()
        return carry

    lax.fori_loop(0, n_cols, drain, 0)

    def drain_reduce(n, carry):
        sib_copy(n).wait_send()
        for copy in z_copies(n) + acc_copies(n):
            copy.wait_send()
        return carry

    lax.fori_loop(0, n_blocks, drain_reduce, 0)
    for copy in waits + ids_copies + count_copies:
        copy.wait_send()


def local(row_ids, table, means, precisions, mix_logits, step_index):
    comps, width = means.shape
    n_comp, n_dp = lax.axis_size("comp"), lax.axis_size("dp")
    share = table.shape[0] // n_dp
    rows = share * n_comp
    n_ids = row_ids.shape[0]
    tile = 256
    blocks = 2 * width // tile
    n_cols = width // tile
    half = comps // NC
    q = half // NH
    packed = 2 * rows + 256
    vmem = pltpu.VMEM
    dma = pltpu.SemaphoreType.DMA
    space = pl.BlockSpec(memory_space=pltpu.VMEM)
    new_means, new_precisions, new_logits = pl.pallas_call(
        kernel,
        out_shape=(
            jax.ShapeDtypeStruct((comps, width), F32),
            jax.ShapeDtypeStruct((comps, width), F32),
            jax.ShapeDtypeStruct((1, comps), F32),
        ),
        in_specs=[space, pl.BlockSpec(memory_space=pl.ANY), space, space, space,
                  pl.BlockSpec(memory_space=pltpu.SMEM)],
        out_specs=(space, space, space),
        scratch_shapes=[
            vmem((n_comp, share, width), F32),
            vmem((n_dp, 1, n_ids), jnp.int32),
            vmem((comps, 2 * width), BF16),
            vmem((comps, 2 * width), BF16),
            vmem((rows, 2 * width), BF16),
            vmem((rows, 2 * width), BF16),
            vmem((comps, rows), F32),
            vmem((comps, rows), BF16),
            vmem((comps, rows), BF16),
            vmem((comps, 1), F32),
            vmem((1, rows), F32),
            vmem((1, rows), F32),
            vmem((NX, 1, packed), F32),
            vmem((NY, 1, packed), F32),
            vmem((NZ, 1, packed), F32),
            vmem((n_dp, 1, comps), F32),
            vmem((comps, 8), F32),
            vmem((blocks, half, tile), F32),
            vmem((blocks, half, tile), F32),
            vmem((blocks, half, tile), F32),
            vmem((blocks, q, tile // 2), F32),
            vmem((blocks, q, tile // 2), F32),
            vmem((blocks, q, tile), F32),
            vmem((blocks, q, tile), F32),
            dma((1,)), dma((n_dp,)), dma((n_dp,)), dma((64 + 8,)), dma((n_comp, 2)),
            dma((3,)), dma((NX,)), dma((3,)), dma((NY,)), dma((1,)), dma((NZ,)), dma((n_dp,)), dma((n_dp,)),
            dma((blocks,)), dma((blocks,)), dma((blocks, 2)), dma((blocks, 2)), dma((blocks, 2)),
            dma((blocks, 2)), dma((blocks, 2)), dma((blocks, 2)),
            dma((n_cols, 2, 2)), dma((n_cols, 2, 3)), dma((n_cols, 2)), dma((n_cols, 2, 4)), dma((n_cols, 2, 4)),
        ],
        compiler_params=pltpu.CompilerParams(
            collective_id=0, has_side_effects=True, vmem_limit_bytes=58 * 2**20
        ),
        name="em",
    )(row_ids.reshape(1, n_ids), table, means, precisions, mix_logits.reshape(1, comps), step_index)
    return new_means, new_precisions, new_logits.reshape(comps)


def solution(mesh):
    placed = (P("dp"), P("comp", None), P("comp", None), P("comp", None), P("comp"), P())
    return jax.shard_map(
        local,
        mesh=mesh,
        in_specs=placed,
        out_specs=(P("comp", None), P("comp", None), P("comp")),
        check_vma=False,
    )
```

```python
import functools

import jax
import jax.numpy as jnp
from jax import lax
from jax.experimental import pallas as pl
from jax.experimental.pallas import tpu as pltpu
from jax.sharding import PartitionSpec as P

F32, BF16 = jnp.float32, jnp.bfloat16
NX, NZ, NY = 4, 2, 4
NH, NC = 4, 2
ROUNDS = ((0, 24), (24, 8))
LANES = (((1,), (1,)), ((), ()))
INNER = (((1,), (0,)), ((), ()))


def split(value):
    high = value.astype(BF16)
    return high, (value - high.astype(F32)).astype(BF16)


def mul(left, right, dims, precision=None):
    return lax.dot_general(left, right, dims, precision=precision, preferred_element_type=F32)


class Copy:
    def __init__(self, src, dst, send_sem, recv_sem, to):
        self.make = lambda: pltpu.make_async_remote_copy(
            src_ref=src, dst_ref=dst, send_sem=send_sem, recv_sem=recv_sem, device_id={"dp": to}
        )

    def start(self):
        self.make().start()

    def wait_send(self):
        self.make().wait_send()

    def wait_recv(self):
        self.make().wait_recv()


def kernel(
    ids_ref, table_ref, means_hbm, prec_hbm, logits_ref, step_ref,
    out_m, out_p, out_mass,
    means_ref, prec_ref, stage, rows, ids_all, a_hi, a_lo, f_hi, f_lo, score, r_hi, r_lo, offset, tops, times_ref, counts_col,
    xb0, yb0, zb0, xb1, yb1, zb1, counts_all, columns,
    sib_out, sib_in, part, from_r, from_l, own_r, own_l,
    local_sem, ids_send, ids_recv, row_send, row_recv, xs, xr, ys, yr, zs, zr, cs, cr,
    sib_s, sib_r, opp_s, opp_r, dir_s, dir_r, acc_s, acc_r,
    gz_s, gz_r, gf_s, gs_s, gs_r, gl_s,
):
    dp, comp = lax.axis_index("dp"), lax.axis_index("comp")
    h, core = dp // NC, dp % NC
    x, zl, y = comp // (NZ * NY), (comp // NY) % NZ, comp % NY
    n_dp = NH * NC
    share = rows.shape[1]
    comps, width = means_ref.shape
    n_rows = f_hi.shape[0]

    def at(dx, dz, dy):
        return ((x + dx) % NX) * (NZ * NY) + ((zl + dz) % NZ) * NY + (y + dy) % NY

    def dp_at(dh, dc):
        return ((h + dh) % NH) * NC + (core + dc) % NC

    peers_c = [at(d, 0, 0) for d in (1, 2, 3)] + [at(0, 0, d) for d in (1, 2, 3)] + [at(0, 1, 0)]
    peers_d = [dp_at(a, b) for a in range(NH) for b in range(NC) if (a, b) != (0, 0)]
    for k, (src, dst) in enumerate(((means_hbm, means_ref), (prec_hbm, prec_ref))):
        pltpu.make_async_copy(src, dst, local_sem.at[1 + k]).start()
    barrier = pltpu.get_barrier_semaphore()
    for peer in peers_c:
        pl.semaphore_signal(barrier, inc=1, device_id={"comp": peer})
    for peer in peers_d:
        pl.semaphore_signal(barrier, inc=1, device_id={"dp": peer})
    pl.semaphore_wait(barrier, len(peers_c) + len(peers_d))

    waits = []

    def send(src, dst, send_sem, recv_sem, **where):
        copy = pltpu.make_async_remote_copy(
            src_ref=src, dst_ref=dst, send_sem=send_sem, recv_sem=recv_sem, device_id=where
        )
        copy.start()
        return copy

    me = at(0, 0, 0)
    mine = pltpu.make_async_copy(table_ref.at[pl.ds(dp * share, share)], rows.at[me], local_sem.at[0])
    mine.start()
    sends = [0]
    first = [(1, 0, 0), (-1, 0, 0)], [(0, 0, 1), (0, 0, -1)]
    wide = width // 2

    def piece(slot, b, t):
        off, size = ROUNDS[t]
        return rows.at[slot, pl.ds(off, size), pl.ds(b * wide, wide)]

    def push(slot, b, t, dx, dz, dy, source=None):
        src = piece(slot, b, t) if source is None else source
        k = sends[0]
        sends[0] += 1
        waits.append(
            send(src, piece(slot, b, t), row_send.at[k], row_recv.at[slot, b, t], comp=at(dx, dz, dy))
        )

    def arrived(slot, b, t):
        pltpu.make_async_copy(piece(slot, b, t), piece(slot, b, t), row_recv.at[slot, b, t]).wait()

    def vec(d, b):
        return (d, 0) if b == 0 else (0, d)

    def own(t):
        off, size = ROUNDS[t]
        src = [table_ref.at[pl.ds(dp * share + off, size), pl.ds(b * wide, wide)] for b in (0, 1)]
        for b in (0, 1):
            push(me, b, t, 0, 1, 0, src[b])
        for k in (0, 1):
            for b in (0, 1):
                for to in first[b ^ k]:
                    push(me, b, t, *to, src[b])

    def partner(t):
        slot = at(0, 1, 0)
        for b in (0, 1):
            arrived(slot, b, t)
            for to in first[b] + first[1 - b]:
                push(slot, b, t, *to)

    def first_near(t):
        for rel in (0, 1):
            for b in (0, 1):
                for d in (-1, 1):
                    dx, dy = vec(d, b)
                    slot = at(dx, rel, dy)
                    arrived(slot, b, t)
                    if (rel == 0) == (d == -1):
                        fx, fy = vec(-d, b)
                        push(slot, b, t, fx, 0, fy)
                    for to in first[1 - b]:
                        push(slot, b, t, *to)

    def first_far(t):
        for rel in (0, 1):
            for b in (0, 1):
                dx, dy = vec(2, b)
                slot = at(dx, rel, dy)
                arrived(slot, b, t)
                for to in first[1 - b]:
                    push(slot, b, t, *to)

    def second_near(t, e):
        for rel in (0, 1):
            for b in (0, 1):
                ex, ey = vec(e, b)
                for d in (-1, 1):
                    dx, dy = vec(d, 1 - b)
                    slot = at(ex + dx, rel, ey + dy)
                    arrived(slot, b, t)
                    if (rel == 0) == (d == -1):
                        fx, fy = vec(-d, 1 - b)
                        push(slot, b, t, fx, 0, fy)

    def second_far(t, e):
        for rel in (0, 1):
            for b in (0, 1):
                ex, ey = vec(e, b)
                dx, dy = vec(2, 1 - b)
                arrived(at(ex + dx, rel, ey + dy), b, t)

    own(0)
    own(1)
    ids_copies = [
        send(ids_ref, ids_all.at[dp], ids_send.at[k], ids_recv.at[dp], dp=peer)
        for k, peer in enumerate(peers_d)
    ]
    ids_all[dp] = ids_ref[...]

    row_block = 32

    def factors(i, carry):
        at_rows = pl.ds(pl.multiple_of(i * row_block, row_block), row_block)
        p, m = prec_ref[at_rows, :], means_ref[at_rows, :]
        cross = p * m
        hi, lo = split(cross)
        a_hi[at_rows, :width], a_lo[at_rows, :width] = hi, lo
        hi, lo = split(-0.5 * (p - 1.0))
        a_hi[at_rows, width:], a_lo[at_rows, width:] = hi, lo
        offset[at_rows, :] = 0.5 * jnp.sum(jnp.log(p) - cross * m, axis=1, keepdims=True)
        return carry

    n_factor = comps // row_block
    partner(0)
    for k, (src, dst) in enumerate(((means_hbm, means_ref), (prec_hbm, prec_ref))):
        pltpu.make_async_copy(src, dst, local_sem.at[1 + k]).wait()
    lax.fori_loop(0, n_factor // 4, factors, 0)
    first_near(0)
    lax.fori_loop(n_factor // 4, n_factor // 2, factors, 0)
    first_far(0)
    partner(1)
    second_near(0, 0)
    lax.fori_loop(n_factor // 2, n_factor, factors, 0)
    logits = logits_ref[...]
    turned = jnp.transpose(jnp.broadcast_to(logits, (8, comps)))
    offset[...] = offset[...] + turned[:, 0:1]
    second_near(0, -1)
    second_near(0, 1)
    first_near(1)

    owners = NX * NZ * NY
    found = jnp.zeros((owners, share), F32)
    for k, peer in enumerate(peers_d):
        pltpu.make_async_copy(ids_ref, ids_all.at[peer], ids_recv.at[peer]).wait()
    per_owner = n_dp * share
    for k in range(n_dp):
        ids = ids_all[k]
        owner = ids // per_owner
        row = ids - owner * per_owner - dp * share
        left = lax.broadcasted_iota(jnp.int32, (owners, ids.shape[1]), 0) == owner
        right = lax.broadcasted_iota(jnp.int32, (share, ids.shape[1]), 0) == row
        found += mul(left.astype(F32).astype(BF16), right.astype(F32).astype(BF16), LANES)
    bases = [owners * off for off, _ in ROUNDS]
    counted = [owners * size for _, size in ROUNDS]
    for (off, size), base, n in zip(ROUNDS, bases, counted):
        flat = lax.broadcasted_iota(jnp.int32, (owners, n), 1)
        pick = (flat // size == lax.broadcasted_iota(jnp.int32, (owners, n), 0)).astype(F32)
        spread_out = mul(found, pick, (((0,), (0,)), ((), ())), lax.Precision.HIGHEST)
        row_of = lax.broadcasted_iota(jnp.int32, (share, n), 0)
        row_flat = lax.broadcasted_iota(jnp.int32, (share, n), 1)
        times_ref[:, base : base + n] = jnp.sum(
            jnp.where(row_flat % size + off == row_of, spread_out, 0.0), axis=0, keepdims=True
        )

    second_near(0, 2)
    first_far(1)
    for e in (0, -1, 1, 2):
        second_far(0, e)
    mine.wait()

    chunk, tile = 256, 256
    packs = ((xb0, yb0, zb0), (xb1, yb1, zb1))

    def scores_of(t, c):
        base, n = bases[t], counted[t]
        cols = slice(base + c * chunk, base + (c + 1) * chunk)

        def block(k, top):
            here = pl.ds(pl.multiple_of(k * tile, tile), tile)
            fh, fl = f_hi[cols, :], f_lo[cols, :]
            s = mul(a_hi[here, :], fh, LANES) + mul(a_hi[here, :], fl, LANES) + mul(a_lo[here, :], fh, LANES)
            s = s + offset[here, :]
            score[here, cols] = s
            return jnp.maximum(top, jnp.max(s, axis=0, keepdims=True))

        top = lax.fori_loop(0, comps // tile, block, jnp.full((1, chunk), -jnp.inf, F32))

        def raise_block(k, mass):
            here = pl.ds(pl.multiple_of(k * 64, 64), 64)
            e = jnp.exp(score[here, cols] - top)
            score[here, cols] = e
            return mass + jnp.sum(e, axis=0, keepdims=True)

        mass = lax.fori_loop(0, comps // 64, raise_block, jnp.zeros((1, chunk), F32))
        tops[:, cols] = top
        packs[t][0][x, :, c * chunk : (c + 1) * chunk] = top
        packs[t][0][x, :, n + c * chunk : n + (c + 1) * chunk] = mass

    def features_of(t):
        off, size = ROUNDS[t]
        base, pair = bases[t], 2 * size

        def features(k, carry):
            s = jnp.concatenate([rows[2 * k, off : off + size, :], rows[2 * k + 1, off : off + size, :]], axis=0)
            here = pl.ds(pl.multiple_of(base + k * pair, 16), pair)
            f_hi[here, :width], f_lo[here, :width] = split(s)
            f_hi[here, width:], f_lo[here, width:] = split(s * s)
            return carry

        lax.fori_loop(0, owners // 2, features, 0)

    logit_top = jnp.max(logits)
    logit_raised = jnp.exp(logits - logit_top)

    def parts_of(t):
        n = counted[t]
        return ((0, n, n), (2 * n, 128, 128)) if t == 0 else ((0, n, n),)

    def combine(ref, n, t):
        out = []
        for start, size, gap in parts_of(t):
            ts = [ref[k, :, start : start + size] for k in range(n)]
            ms = [ref[k, :, start + gap : start + gap + size] for k in range(n)]
            top = functools.reduce(jnp.maximum, ts)
            out.append((start, size, gap, top, sum(m * jnp.exp(a - top) for m, a in zip(ms, ts))))
        return out

    def fill(ref, index, results):
        for start, size, gap, top, m in results:
            ref[index, :, start : start + size] = top
            ref[index, :, start + gap : start + gap + size] = m

    to_x, to_y, to_z = [at(d, 0, 0) for d in (1, 2, 3)], [at(0, 0, d) for d in (1, 2, 3)], [at(0, 1, 0)]
    from_x, from_y, from_z = [(x + d) % NX for d in (1, 2, 3)], [(y + d) % NY for d in (1, 2, 3)], [(zl + 1) % NZ]
    stages = ((x, to_x, from_x, xs, xr), (y, to_y, from_y, ys, yr), (zl, to_z, from_z, zs, zr))

    def stage_send(t, d):
        ref, (index, to, _, s_sem, r_sem) = packs[t][d], stages[d]
        for k, peer in enumerate(to):
            waits.append(send(ref.at[index], ref.at[index], s_sem.at[t, k], r_sem.at[t, index], comp=peer))

    def stage_wait(t, d):
        ref, (_, _, slots, _, r_sem) = packs[t][d], stages[d]
        for slot in slots:
            pltpu.make_async_copy(ref.at[slot], ref.at[slot], r_sem.at[t, slot]).wait()
        return combine(ref, (NX, NY, NZ)[d], t)

    def stage_next(t, d):
        fill(packs[t][d + 1], stages[d + 1][0], stage_wait(t, d))
        stage_send(t, d + 1)

    features_of(0)
    n_chunks = counted[0] // chunk
    for c in range(n_chunks):
        scores_of(0, c)
        if c == 0:
            second_near(1, 0)
            second_near(1, -1)
        elif c == 1:
            second_near(1, 1)
            second_near(1, 2)
    xb0[x, :, 2 * counted[0] : 2 * counted[0] + 128] = jnp.full((1, 128), logit_top, F32)
    xb0[x, :, 2 * counted[0] + 128 :] = jnp.full((1, 128), jnp.sum(logit_raised), F32)
    stage_send(0, 0)
    for e in (0, -1, 1, 2):
        second_far(1, e)
    features_of(1)
    stage_next(0, 0)
    scores_of(1, 0)
    stage_send(1, 0)
    stage_next(0, 1)

    def responsibilities(t, peak, total):
        cols = slice(bases[t], bases[t] + counted[t])
        factor = jnp.exp(tops[:, cols] - peak) / total * times_ref[:, cols]

        def one(k, carry):
            here = pl.ds(pl.multiple_of(k * row_block, row_block), row_block)
            r = score[here, cols] * factor
            r_hi[here, cols], r_lo[here, cols] = split(r)
            found = jnp.sum(r, axis=1, keepdims=True)
            counts_col[here, :] = found if t == 0 else counts_col[here, :] + found
            return carry

        lax.fori_loop(0, comps // row_block, one, 0)

    n_blocks = 2 * width // tile
    own_half = comps // NC
    q = own_half // NH
    side = tile // 2
    L, R = dp_at(-1, 0), dp_at(1, 0)
    sib = dp_at(0, 1)

    def moment(n, which, t):
        start = pl.multiple_of((n % 2) * width + (n // 2) * tile, tile)
        cols = pl.ds(start, tile)
        here = pl.ds(pl.multiple_of(which * own_half, own_half), own_half)
        deep = slice(bases[t], bases[t] + counted[t])
        fh, fl, rh = f_hi[deep, cols], f_lo[deep, cols], r_hi[here, deep]
        return mul(rh, fh, INNER) + mul(rh, fl, INNER) + mul(r_lo[here, deep], fh, INNER)

    def early(n, carry):
        sib_out[n] = moment(n, 1 - core, 0)
        part[n] = moment(n, core, 0)
        return carry

    (_, _, _, peak, total), (_, _, _, logit_peak, logit_total) = stage_wait(0, 2)
    responsibilities(0, peak, total)
    stage_next(1, 0)
    lax.fori_loop(0, n_blocks // 2, early, 0)
    stage_next(1, 1)
    lax.fori_loop(n_blocks // 2, n_blocks, early, 0)
    ((_, _, _, peak, total),) = stage_wait(1, 2)
    responsibilities(1, peak, total)

    def sib_copy(n):
        return Copy(sib_out.at[n], sib_in.at[n], sib_s.at[n], sib_r.at[n], sib)

    def for_sibling(n):
        sib_out[n] = sib_out[n] + moment(n, 1 - core, 1)
        sib_copy(n).start()

    def chunk_of(n, o, b):
        return part.at[n, pl.ds(pl.multiple_of(o * q, q), q), pl.ds(b * side, side)]

    left_h, right_h, far_h = (h - 1) % NH, (h + 1) % NH, (h + 2) % NH

    def remote(src, dst, s, r, to):
        return Copy(src, dst, s, r, to)

    def cols_of(b):
        return pl.ds(b * side, side)

    def z_copies(n):
        return [
            remote(chunk_of(n, far_h, 0), from_r.at[n], opp_s.at[n, 0], opp_r.at[n, 0], L),
            remote(chunk_of(n, far_h, 1), from_l.at[n], opp_s.at[n, 1], opp_r.at[n, 1], R),
            remote(chunk_of(n, left_h, 1), own_r.at[n, :, cols_of(1)], dir_s.at[n, 0], dir_r.at[n, 0], L),
            remote(chunk_of(n, right_h, 0), own_l.at[n, :, cols_of(0)], dir_s.at[n, 1], dir_r.at[n, 1], R),
        ]

    def acc_copies(n):
        return [
            remote(chunk_of(n, left_h, 0), own_r.at[n, :, cols_of(0)], acc_s.at[n, 0], acc_r.at[n, 0], L),
            remote(chunk_of(n, right_h, 1), own_l.at[n, :, cols_of(1)], acc_s.at[n, 1], acc_r.at[n, 1], R),
        ]

    def relay(n):
        opp, acc = z_copies(n)[:2], acc_copies(n)
        opp[0].wait_recv()
        spot = chunk_of(n, left_h, 0)
        spot[...] = spot[...] + from_r[n]
        acc[0].start()
        opp[1].wait_recv()
        spot = chunk_of(n, right_h, 1)
        spot[...] = spot[...] + from_l[n]
        acc[1].start()

    for_sibling(0)
    counts_all[dp] = jnp.transpose(jnp.broadcast_to(counts_col[...], (comps, 8)))[0:1, :]
    count_copies = [
        send(counts_all.at[dp], counts_all.at[dp], cs.at[k], cr.at[dp], dp=peer)
        for k, peer in enumerate(peers_d)
    ]

    def reduce_step(n, carry):
        @pl.when(n + 1 < n_blocks)
        def _():
            for_sibling(n + 1)

        own_block = part[n] + moment(n, core, 1)
        sib_copy(n).wait_recv()
        part[n] = own_block + sib_in[n]
        for copy in z_copies(n):
            copy.start()

        @pl.when(n > 0)
        def _():
            relay(n - 1)

        return carry

    lax.fori_loop(0, n_blocks, reduce_step, 0)
    relay(n_blocks - 1)

    for k, peer in enumerate(peers_d):
        pltpu.make_async_copy(counts_all.at[peer], counts_all.at[peer], cr.at[peer]).wait()
    counts = sum(counts_all[k] for k in range(n_dp))
    batch = 1.0 * n_dp * ids_ref.shape[1]
    index = jnp.full((1, comps), step_ref[0].astype(F32), F32)
    step = jnp.exp(-0.6 * jnp.log(2.0 + index / 8192.0))
    retain = 1.0 - step
    weights = logit_raised * (jnp.exp(logit_top - logit_peak[:, 0:1]) / logit_total[:, 0:1])
    prior = retain * weights
    mass_new = prior + step * counts / batch
    out_mass[...] = mass_new
    stacked = jnp.concatenate([mass_new, prior, counts, step, mass_new, prior, counts, step], axis=0)
    columns[...] = jnp.transpose(stacked)

    mine_at = pl.ds(pl.multiple_of(core * own_half + h * q, q), q)
    col = columns[mine_at, :]
    mass_c, prior_c, counts_c, step_c = (col[:, k : k + 1] for k in range(4))

    def reduced(n):
        z, acc = z_copies(n), acc_copies(n)
        for copy in (z[2], z[3], acc[0], acc[1]):
            copy.wait_recv()
        return part[n, pl.ds(pl.multiple_of(h * q, q), q), :] + own_r[n] + own_l[n]

    outs = (out_m, out_p)

    def out_piece(a, cb, o, c):
        here = pl.ds(pl.multiple_of(c * own_half + o * q, q), q)
        return outs[a].at[here, pl.ds(pl.multiple_of(cb * tile, tile), tile)]

    def own_piece(a, cb):
        return stage.at[a, :, pl.ds(pl.multiple_of(cb * tile, tile), tile)]

    def own_local(cb, a):
        return pltpu.make_async_copy(own_piece(a, cb), out_piece(a, cb, h, core), gl_s.at[cb, a])

    def z_gather(a, cb, o, s, r, to, src=None):
        src = out_piece(a, cb, o, core) if src is None else src
        return remote(src, out_piece(a, cb, o, core), s, r, to)

    def own_sends(cb):
        found = []
        for a in (0, 1):
            found.append(z_gather(a, cb, h, gz_s.at[cb, a, 0], gz_r.at[cb, a, 0], R, own_piece(a, cb)))
            found.append(z_gather(a, cb, h, gz_s.at[cb, a, 1], gz_r.at[cb, a, 1], L, own_piece(a, cb)))
            found.append(z_gather(a, cb, h, gs_s.at[cb, a, 0], gs_r.at[cb, a, 0], sib, own_piece(a, cb)))
        return found

    def forwards(cb):
        return [
            z_gather(0, cb, left_h, gf_s.at[cb, 0], gz_r.at[cb, 0, 2], R),
            z_gather(1, cb, right_h, gf_s.at[cb, 1], gz_r.at[cb, 1, 2], L),
        ]

    def sib_sends(cb, a, k):
        o = (left_h, right_h, far_h)[k]
        return z_gather(a, cb, o, gs_s.at[cb, a, 1 + k], gs_r.at[cb, a, 1 + k], sib)

    def z_arrived(cb, a, k):
        o = (left_h, right_h, far_h)[k]
        ref = out_piece(a, cb, o, core)
        pltpu.make_async_copy(ref, ref, gz_r.at[cb, a, k]).wait()

    def update(cb, carry):
        first_m, second_m = reduced(2 * cb), reduced(2 * cb + 1)
        cols = pl.ds(pl.multiple_of(cb * tile, tile), tile)
        m, p = means_ref[mine_at, cols], prec_ref[mine_at, cols]
        weighted = prior_c * m + step_c * first_m / batch
        new_m = weighted / mass_c
        moved = m - new_m
        spread = (
            prior_c * (1.0 / p + moved * moved)
            + step_c * (second_m - 2.0 * new_m * first_m + new_m * new_m * counts_c) / batch
        )
        stage[0, :, cols] = weighted
        stage[1, :, cols] = spread
        for copy in own_sends(cb):
            copy.start()
        for a in (0, 1):
            own_local(cb, a).start()

        @pl.when(cb > 0)
        def _():
            pass_on(cb - 1)

        return carry

    def pass_on(cb):
        fwd = forwards(cb)
        z_arrived(cb, 0, 0)
        fwd[0].start()
        z_arrived(cb, 1, 1)
        fwd[1].start()
        sib_sends(cb, 0, 0).start()
        sib_sends(cb, 1, 1).start()
        z_arrived(cb, 1, 0)
        sib_sends(cb, 1, 0).start()
        z_arrived(cb, 0, 1)
        sib_sends(cb, 0, 1).start()

    n_cols = width // tile
    lax.fori_loop(0, n_cols, update, 0)
    pass_on(n_cols - 1)

    def finish(cb, carry):
        for a in (0, 1):
            z_arrived(cb, a, 2)
            sib_sends(cb, a, 2).start()
        return carry

    lax.fori_loop(0, n_cols, finish, 0)

    def drain(cb, carry):
        for copy in own_sends(cb) + forwards(cb):
            copy.wait_send()
        for a in (0, 1):
            own_local(cb, a).wait()
            for k in range(3):
                sib_sends(cb, a, k).wait_send()
            for k, o in enumerate((h, left_h, right_h, far_h)):
                ref = out_piece(a, cb, o, 1 - core)
                pltpu.make_async_copy(ref, ref, gs_r.at[cb, a, k]).wait()
        return carry

    lax.fori_loop(0, n_cols, drain, 0)

    def drain_reduce(n, carry):
        sib_copy(n).wait_send()
        for copy in z_copies(n) + acc_copies(n):
            copy.wait_send()
        return carry

    lax.fori_loop(0, n_blocks, drain_reduce, 0)
    for copy in waits + ids_copies + count_copies:
        copy.wait_send()


def local(row_ids, table, means, precisions, mix_logits, step_index):
    comps, width = means.shape
    n_comp, n_dp = lax.axis_size("comp"), lax.axis_size("dp")
    share = table.shape[0] // n_dp
    rows = share * n_comp
    n_ids = row_ids.shape[0]
    tile = 256
    blocks = 2 * width // tile
    n_cols = width // tile
    half = comps // NC
    q = half // NH
    packed = [2 * n_comp * size + (256 if t == 0 else 0) for t, (_, size) in enumerate(ROUNDS)]
    anywhere = pl.BlockSpec(memory_space=pl.ANY)
    vmem = pltpu.VMEM
    dma = pltpu.SemaphoreType.DMA
    space = pl.BlockSpec(memory_space=pltpu.VMEM)
    weighted, spread, mass = pl.pallas_call(
        kernel,
        out_shape=(
            jax.ShapeDtypeStruct((comps, width), F32),
            jax.ShapeDtypeStruct((comps, width), F32),
            jax.ShapeDtypeStruct((1, comps), F32),
        ),
        in_specs=[space, anywhere, anywhere, anywhere, space, pl.BlockSpec(memory_space=pltpu.SMEM)],
        out_specs=(anywhere, anywhere, space),
        scratch_shapes=[
            vmem((comps, width), F32),
            vmem((comps, width), F32),
            vmem((2, q, width), F32),
            vmem((n_comp, share, width), F32),
            vmem((n_dp, 1, n_ids), jnp.int32),
            vmem((comps, 2 * width), BF16),
            vmem((comps, 2 * width), BF16),
            vmem((rows, 2 * width), BF16),
            vmem((rows, 2 * width), BF16),
            vmem((comps, rows), F32),
            vmem((comps, rows), BF16),
            vmem((comps, rows), BF16),
            vmem((comps, 1), F32),
            vmem((1, rows), F32),
            vmem((1, rows), F32),
            vmem((comps, 1), F32),
            *[vmem((n, 1, packed[t]), F32) for t in (0, 1) for n in (NX, NY, NZ)],
            vmem((n_dp, 1, comps), F32),
            vmem((comps, 8), F32),
            vmem((blocks, half, tile), F32),
            vmem((blocks, half, tile), F32),
            vmem((blocks, half, tile), F32),
            vmem((blocks, q, tile // 2), F32),
            vmem((blocks, q, tile // 2), F32),
            vmem((blocks, q, tile), F32),
            vmem((blocks, q, tile), F32),
            dma((3,)), dma((n_dp,)), dma((n_dp,)), dma((2 * 62,)), dma((n_comp, 2, 2)),
            dma((2, 3)), dma((2, NX)), dma((2, 3)), dma((2, NY)), dma((2, 1)), dma((2, NZ)), dma((n_dp,)), dma((n_dp,)),
            dma((blocks,)), dma((blocks,)), dma((blocks, 2)), dma((blocks, 2)), dma((blocks, 2)),
            dma((blocks, 2)), dma((blocks, 2)), dma((blocks, 2)),
            dma((n_cols, 2, 2)), dma((n_cols, 2, 3)), dma((n_cols, 2)), dma((n_cols, 2, 4)), dma((n_cols, 2, 4)), dma((n_cols, 2)),
        ],
        compiler_params=pltpu.CompilerParams(
            collective_id=0, has_side_effects=True, vmem_limit_bytes=58 * 2**20
        ),
        name="em",
    )(row_ids.reshape(1, n_ids), table, means, precisions, mix_logits.reshape(1, comps), step_index)
    mass = mass.reshape(comps)
    return weighted / mass[:, None], mass[:, None] / spread, jnp.log(mass)


def solution(mesh):
    placed = (P("dp"), P("comp", None), P("comp", None), P("comp", None), P("comp"), P())
    return jax.shard_map(
        local,
        mesh=mesh,
        in_specs=placed,
        out_specs=(P("comp", None), P("comp", None), P("comp")),
        check_vma=False,
    )
```

```python
import functools

import jax
import jax.numpy as jnp
from jax import lax
from jax.experimental import pallas as pl
from jax.experimental.pallas import tpu as pltpu
from jax.sharding import PartitionSpec as P

F32, BF16 = jnp.float32, jnp.bfloat16
NX, NZ, NY = 4, 2, 4
NH, NC = 4, 2
LANES = (((1,), (1,)), ((), ()))
INNER = (((1,), (0,)), ((), ()))


def split(value):
    high = value.astype(BF16)
    return high, (value - high.astype(F32)).astype(BF16)


def mul(left, right, dims, precision=None):
    return lax.dot_general(left, right, dims, precision=precision, preferred_element_type=F32)


class Copy:
    def __init__(self, src, dst, send_sem, recv_sem, to):
        self.make = lambda: pltpu.make_async_remote_copy(
            src_ref=src, dst_ref=dst, send_sem=send_sem, recv_sem=recv_sem, device_id={"dp": to}
        )

    def start(self):
        self.make().start()

    def wait_send(self):
        self.make().wait_send()

    def wait_recv(self):
        self.make().wait_recv()


def kernel(
    ids_ref, table_ref, means_hbm, prec_hbm, logits_ref, step_ref,
    out_m, out_p, out_mass,
    means_ref, prec_ref, stage, rows, ids_all, a_hi, a_lo, f_hi, f_lo, score, r_hi, r_lo, offset, tops, times_ref, counts_col,
    xb, yb, peaks, scale, factors_ref, counts_all, columns,
    sib_out, sib_in, part, from_r, from_l, own_r, own_l,
    local_sem, ids_send, ids_recv, row_send, row_recv, xs, xr, ys, yr, cs, cr,
    sib_s, sib_r, opp_s, opp_r, dir_s, dir_r, acc_s, acc_r,
    gz_s, gz_r, gf_s, gs_s, gs_r, gl_s,
):
    dp, comp = lax.axis_index("dp"), lax.axis_index("comp")
    h, core = lax.div(dp, NC), lax.rem(dp, NC)
    x, zl, y = lax.div(comp, NZ * NY), lax.rem(lax.div(comp, NY), NZ), lax.rem(comp, NY)
    x_at = {d: lax.rem(x + (d % NX), NX) for d in (-1, 0, 1, 2, 3)}
    y_at = {d: lax.rem(y + (d % NY), NY) for d in (-1, 0, 1, 2, 3)}
    z_at = {0: zl, 1: 1 - zl}
    h_at = {d: lax.rem(h + (d % NH), NH) for d in (-1, 0, 1, 2, 3)}
    c_at = {0: core, 1: 1 - core}
    n_dp = NH * NC
    share = rows.shape[1]
    comps, width = means_ref.shape
    n_rows = f_hi.shape[0]

    def at(dx, dz, dy):
        return x_at[dx] * (NZ * NY) + z_at[dz] * NY + y_at[dy]

    def dp_at(dh, dc):
        return h_at[dh] * NC + c_at[dc]

    plane = [(a, b) for a in range(NZ) for b in range(NY) if (a, b) != (0, 0)]
    to_x, to_yz = [at(d, 0, 0) for d in (1, 2, 3)], [at(0, a, b) for a, b in plane]
    peers_c = to_x + to_yz
    peers_d = [dp_at(a, b) for a in range(NH) for b in range(NC) if (a, b) != (0, 0)]
    for k, (src, dst) in enumerate(((means_hbm, means_ref), (prec_hbm, prec_ref))):
        pltpu.make_async_copy(src, dst, local_sem.at[1 + k]).start()
    barrier = pltpu.get_barrier_semaphore()
    for peer in peers_c:
        pl.semaphore_signal(barrier, inc=1, device_id={"comp": peer})
    for peer in peers_d:
        pl.semaphore_signal(barrier, inc=1, device_id={"dp": peer})

    row_block = 32

    def factors(i, carry):
        at_rows = pl.ds(pl.multiple_of(i * row_block, row_block), row_block)
        p, m = prec_ref[at_rows, :], means_ref[at_rows, :]
        cross = p * m
        hi, lo = split(cross)
        a_hi[at_rows, :width], a_lo[at_rows, :width] = hi, lo
        hi, lo = split(-0.5 * (p - 1.0))
        a_hi[at_rows, width:], a_lo[at_rows, width:] = hi, lo
        offset[at_rows, :] = 0.5 * jnp.sum(jnp.log(p) - cross * m, axis=1, keepdims=True)
        return carry

    for k, (src, dst) in enumerate(((means_hbm, means_ref), (prec_hbm, prec_ref))):
        pltpu.make_async_copy(src, dst, local_sem.at[1 + k]).wait()
    lax.fori_loop(0, comps // row_block, factors, 0)
    logits = logits_ref[...]
    turned = jnp.transpose(jnp.broadcast_to(logits, (8, comps)))
    offset[...] = offset[...] + turned[:, 0:1]
    pl.semaphore_wait(barrier, len(peers_c) + len(peers_d))

    waits = []

    def send(src, dst, send_sem, recv_sem, **where):
        copy = pltpu.make_async_remote_copy(
            src_ref=src, dst_ref=dst, send_sem=send_sem, recv_sem=recv_sem, device_id=where
        )
        copy.start()
        return copy

    me = at(0, 0, 0)
    mine = pltpu.make_async_copy(table_ref.at[pl.ds(dp * share, share)], rows.at[me], local_sem.at[0])
    mine.start()
    sends = [0]
    first = [(1, 0, 0), (-1, 0, 0)], [(0, 0, 1), (0, 0, -1)]
    half = share // 2

    def piece(slot, b):
        return rows.at[slot, pl.ds(b * half, half)]

    def push(slot, b, dx, dz, dy, source=None):
        src = piece(slot, b) if source is None else source
        k = sends[0]
        sends[0] += 1
        waits.append(
            send(src, piece(slot, b), row_send.at[k], row_recv.at[slot, b], comp=at(dx, dz, dy))
        )

    def arrived(slot, b):
        pltpu.make_async_copy(piece(slot, b), piece(slot, b), row_recv.at[slot, b]).wait()

    def vec(d, b):
        return (d, 0) if b == 0 else (0, d)

    def own():
        src = [table_ref.at[pl.ds(dp * share + b * half, half)] for b in (0, 1)]
        for b in (0, 1):
            push(me, b, 0, 1, 0, src[b])
        for k in (0, 1):
            for b in (0, 1):
                for to in first[b ^ k]:
                    push(me, b, *to, src[b])

    def partner():
        slot = at(0, 1, 0)
        for b in (0, 1):
            arrived(slot, b)
            for to in first[b] + first[1 - b]:
                push(slot, b, *to)

    def first_near():
        for rel in (0, 1):
            for b in (0, 1):
                for d in (-1, 1):
                    dx, dy = vec(d, b)
                    slot = at(dx, rel, dy)
                    arrived(slot, b)
                    if (rel == 0) == (d == -1):
                        fx, fy = vec(-d, b)
                        push(slot, b, fx, 0, fy)
                    for to in first[1 - b]:
                        push(slot, b, *to)

    def first_far():
        for rel in (0, 1):
            for b in (0, 1):
                dx, dy = vec(2, b)
                slot = at(dx, rel, dy)
                arrived(slot, b)
                for to in first[1 - b]:
                    push(slot, b, *to)

    def second_near(e):
        for rel in (0, 1):
            for b in (0, 1):
                ex, ey = vec(e, b)
                for d in (-1, 1):
                    dx, dy = vec(d, 1 - b)
                    slot = at(ex + dx, rel, ey + dy)
                    arrived(slot, b)
                    if (rel == 0) == (d == -1):
                        fx, fy = vec(-d, 1 - b)
                        push(slot, b, fx, 0, fy)

    def second_far(e):
        for rel in (0, 1):
            for b in (0, 1):
                ex, ey = vec(e, b)
                dx, dy = vec(2, 1 - b)
                arrived(at(ex + dx, rel, ey + dy), b)

    own()
    ids_copies = [
        send(ids_ref, ids_all.at[dp], ids_send.at[k], ids_recv.at[dp], dp=peer)
        for k, peer in enumerate(peers_d)
    ]
    ids_all[dp] = ids_ref[...]

    partner()
    first_near()
    first_far()
    second_near(0)

    owners = NX * NZ * NY
    found = jnp.zeros((owners, share), F32)
    for k, peer in enumerate(peers_d):
        pltpu.make_async_copy(ids_ref, ids_all.at[peer], ids_recv.at[peer]).wait()
    per_owner = n_dp * share
    for k in range(n_dp):
        ids = ids_all[k]
        owner = ids // per_owner
        row = ids - owner * per_owner - dp * share
        left = lax.broadcasted_iota(jnp.int32, (owners, ids.shape[1]), 0) == owner
        right = lax.broadcasted_iota(jnp.int32, (share, ids.shape[1]), 0) == row
        found += mul(left.astype(F32).astype(BF16), right.astype(F32).astype(BF16), LANES)
    flat = lax.broadcasted_iota(jnp.int32, (owners, n_rows), 1)
    slot_of = lax.broadcasted_iota(jnp.int32, (owners, n_rows), 0)
    later = flat - owners * half
    along_x = lax.div(flat, half)
    xz = lax.rem(lax.div(later, half), NX * NZ)
    along_y = xz * NY + lax.div(later, NX * NZ * half)
    pick = (jnp.where(later < 0, along_x, along_y) == slot_of).astype(F32)
    spread_out = mul(found, pick, (((0,), (0,)), ((), ())), lax.Precision.HIGHEST)
    row_of = lax.broadcasted_iota(jnp.int32, (share, n_rows), 0)
    row_flat = lax.broadcasted_iota(jnp.int32, (share, n_rows), 1)
    row_flat = lax.rem(row_flat, half) + jnp.where(row_flat < owners * half, 0, half)
    times_ref[...] = jnp.sum(jnp.where(row_flat == row_of, spread_out, 0.0), axis=0, keepdims=True)

    tile = 256
    block_cols = owners * half // NX
    chunk = 2 * block_cols
    order = (0, -1, 1, 2)

    def places(e):
        return (
            pl.multiple_of(x_at[e] * block_cols, block_cols),
            pl.multiple_of(owners * half + y_at[e] * block_cols, block_cols),
        )

    def features_of(e):
        base = order.index(e) * chunk

        def features(k, carry):
            slots = (x_at[e] * (NZ * NY) + k, k * NY + y_at[e])
            for b in (0, 1):
                s = rows[slots[b], b * half : (b + 1) * half, :]
                here = pl.ds(pl.multiple_of(base + b * block_cols + k * half, half), half)
                f_hi[here, :width], f_lo[here, :width] = split(s)
                f_hi[here, width:], f_lo[here, width:] = split(s * s)
            return carry

        lax.fori_loop(0, NZ * NY, features, 0)

    def scores_of(e):
        base = order.index(e) * chunk
        cols = slice(base, base + chunk)

        def block(k, top):
            here = pl.ds(pl.multiple_of(k * tile, tile), tile)
            fh, fl = f_hi[cols, :], f_lo[cols, :]
            s = mul(a_hi[here, :], fh, LANES) + mul(a_hi[here, :], fl, LANES) + mul(a_lo[here, :], fh, LANES)
            s = s + offset[here, :]
            score[here, cols] = s
            return jnp.maximum(top, jnp.max(s, axis=0, keepdims=True))

        top = lax.fori_loop(0, comps // tile, block, jnp.full((1, chunk), -jnp.inf, F32))

        def raise_block(k, mass):
            here = pl.ds(pl.multiple_of(k * 64, 64), 64)
            e = jnp.exp(score[here, cols] - top)
            score[here, cols] = e
            return mass + jnp.sum(e, axis=0, keepdims=True)

        mass = lax.fori_loop(0, comps // 64, raise_block, jnp.zeros((1, chunk), F32))
        tops[:, cols] = top
        for b, place in enumerate(places(e)):
            part_cols = slice(b * block_cols, (b + 1) * block_cols)
            xb[x, :, pl.ds(place, block_cols)] = top[:, part_cols]
            xb[x, :, pl.ds(pl.multiple_of(n_rows + place, block_cols), block_cols)] = mass[:, part_cols]

    logit_top = jnp.max(logits)
    logit_raised = jnp.exp(logits - logit_top)

    parts = ((0, n_rows, n_rows), (2 * n_rows, 128, 128))

    def combine(ref, n):
        out = []
        for start, size, gap in parts:
            ts = [ref[k, :, start : start + size] for k in range(n)]
            ms = [ref[k, :, start + gap : start + gap + size] for k in range(n)]
            top = functools.reduce(jnp.maximum, ts)
            out.append((start, size, gap, top, sum(m * jnp.exp(a - top) for m, a in zip(ms, ts))))
        return out

    def fill(ref, index, results):
        for start, size, gap, top, m in results:
            ref[index, :, start : start + size] = top
            ref[index, :, start + gap : start + gap + size] = m

    from_x = [x_at[d] for d in (1, 2, 3)]
    from_yz = [z_at[a] * NY + y_at[b] for a, b in plane]
    stages = ((x, to_x, from_x, xs, xr), (zl * NY + y, to_yz, from_yz, ys, yr))

    packs = (xb, yb)

    def stage_send(d):
        ref, (index, to, _, s_sem, r_sem) = packs[d], stages[d]
        for k, peer in enumerate(to):
            waits.append(send(ref.at[index], ref.at[index], s_sem.at[k], r_sem.at[index], comp=peer))

    def stage_wait(d):
        ref, (_, _, slots, _, r_sem) = packs[d], stages[d]
        for slot in slots:
            pltpu.make_async_copy(ref.at[slot], ref.at[slot], r_sem.at[slot]).wait()
        return combine(ref, (NX, NZ * NY)[d])

    xb[x, :, 2 * n_rows : 2 * n_rows + 128] = jnp.full((1, 128), logit_top, F32)
    xb[x, :, 2 * n_rows + 128 :] = jnp.full((1, 128), jnp.sum(logit_raised), F32)
    second_near(-1)
    second_far(0)
    mine.wait()
    features_of(0)
    scores_of(0)
    second_near(1)
    second_near(2)
    for e in (-1, 1, 2):
        second_far(e)
        features_of(e)
        scores_of(e)
    stage_send(0)
    fill(yb, stages[1][0], stage_wait(0))
    stage_send(1)
    (_, _, _, peak, total), (_, _, _, logit_peak, logit_total) = stage_wait(1)

    peaks[...] = peak
    scale[...] = times_ref[...] / total
    for k, e in enumerate(order):
        for b, place in enumerate(places(e)):
            cols = slice(k * chunk + b * block_cols, k * chunk + (b + 1) * block_cols)
            at_place = pl.ds(place, block_cols)
            factors_ref[:, cols] = jnp.exp(tops[:, cols] - peaks[:, at_place]) * scale[:, at_place]
    factor = factors_ref[...]

    def responsibilities(which):
        def one(k, carry):
            here = pl.ds(pl.multiple_of(which * (comps // NC) + k * row_block, row_block), row_block)
            r = score[here, :] * factor
            r_hi[here, :], r_lo[here, :] = split(r)
            counts_col[here, :] = jnp.sum(r, axis=1, keepdims=True)
            return carry

        lax.fori_loop(0, comps // NC // row_block, one, 0)

    n_blocks = 2 * width // tile
    own_half = comps // NC
    q = own_half // NH
    side = tile // 2
    L, R = dp_at(-1, 0), dp_at(1, 0)
    sib = dp_at(0, 1)

    def moment(n, which):
        start = pl.multiple_of(lax.rem(n, 2) * width + lax.div(n, 2) * tile, tile)
        cols = pl.ds(start, tile)
        here = pl.ds(pl.multiple_of(which * own_half, own_half), own_half)
        fh, fl, rh = f_hi[:, cols], f_lo[:, cols], r_hi[here, :]
        return mul(rh, fh, INNER) + mul(rh, fl, INNER) + mul(r_lo[here, :], fh, INNER)

    def sib_copy(n):
        return Copy(sib_out.at[n], sib_in.at[n], sib_s.at[n], sib_r.at[n], sib)

    def for_sibling(n):
        sib_out[n] = moment(n, 1 - core)
        sib_copy(n).start()

    def chunk_of(n, o, b):
        return part.at[n, pl.ds(pl.multiple_of(o * q, q), q), pl.ds(b * side, side)]

    left_h, right_h, far_h = h_at[-1], h_at[1], h_at[2]

    def remote(src, dst, s, r, to):
        return Copy(src, dst, s, r, to)

    def cols_of(b):
        return pl.ds(b * side, side)

    def z_copies(n):
        return [
            remote(chunk_of(n, far_h, 0), from_r.at[n], opp_s.at[n, 0], opp_r.at[n, 0], L),
            remote(chunk_of(n, far_h, 1), from_l.at[n], opp_s.at[n, 1], opp_r.at[n, 1], R),
            remote(chunk_of(n, left_h, 1), own_r.at[n, :, cols_of(1)], dir_s.at[n, 0], dir_r.at[n, 0], L),
            remote(chunk_of(n, right_h, 0), own_l.at[n, :, cols_of(0)], dir_s.at[n, 1], dir_r.at[n, 1], R),
        ]

    def acc_copies(n):
        return [
            remote(chunk_of(n, left_h, 0), own_r.at[n, :, cols_of(0)], acc_s.at[n, 0], acc_r.at[n, 0], L),
            remote(chunk_of(n, right_h, 1), own_l.at[n, :, cols_of(1)], acc_s.at[n, 1], acc_r.at[n, 1], R),
        ]

    def relay(n):
        opp, acc = z_copies(n)[:2], acc_copies(n)
        opp[0].wait_recv()
        spot = chunk_of(n, left_h, 0)
        spot[...] = spot[...] + from_r[n]
        acc[0].start()
        opp[1].wait_recv()
        spot = chunk_of(n, right_h, 1)
        spot[...] = spot[...] + from_l[n]
        acc[1].start()

    responsibilities(1 - core)
    for_sibling(0)
    responsibilities(core)
    counts_all[dp] = jnp.transpose(jnp.broadcast_to(counts_col[...], (comps, 8)))[0:1, :]
    count_copies = [
        send(counts_all.at[dp], counts_all.at[dp], cs.at[k], cr.at[dp], dp=peer)
        for k, peer in enumerate(peers_d)
    ]

    def reduce_step(n, carry):
        @pl.when(n + 1 < n_blocks)
        def _():
            for_sibling(n + 1)

        own_block = moment(n, core)
        sib_copy(n).wait_recv()
        part[n] = own_block + sib_in[n]
        for copy in z_copies(n):
            copy.start()

        @pl.when(n > 0)
        def _():
            relay(n - 1)

        return carry

    lax.fori_loop(0, n_blocks, reduce_step, 0)
    relay(n_blocks - 1)

    for k, peer in enumerate(peers_d):
        pltpu.make_async_copy(counts_all.at[peer], counts_all.at[peer], cr.at[peer]).wait()
    counts = sum(counts_all[k] for k in range(n_dp))
    batch = 1.0 * n_dp * ids_ref.shape[1]
    index = jnp.full((1, comps), step_ref[0].astype(F32), F32)
    step = jnp.exp(-0.6 * jnp.log(2.0 + index / 8192.0))
    retain = 1.0 - step
    weights = logit_raised * (jnp.exp(logit_top - logit_peak[:, 0:1]) / logit_total[:, 0:1])
    prior = retain * weights
    mass_new = prior + step * counts / batch
    out_mass[...] = mass_new
    stacked = jnp.concatenate([mass_new, prior, counts, step, mass_new, prior, counts, step], axis=0)
    columns[...] = jnp.transpose(stacked)

    mine_at = pl.ds(pl.multiple_of(core * own_half + h * q, q), q)
    col = columns[mine_at, :]
    mass_c, prior_c, counts_c, step_c = (col[:, k : k + 1] for k in range(4))

    def reduced(n):
        z, acc = z_copies(n), acc_copies(n)
        for copy in (z[2], z[3], acc[0], acc[1]):
            copy.wait_recv()
        return part[n, pl.ds(pl.multiple_of(h * q, q), q), :] + own_r[n] + own_l[n]

    outs = (out_m, out_p)

    def out_piece(a, cb, o, c):
        here = pl.ds(pl.multiple_of(c * own_half + o * q, q), q)
        return outs[a].at[here, pl.ds(pl.multiple_of(cb * tile, tile), tile)]

    def own_piece(a, cb):
        return stage.at[a, :, pl.ds(pl.multiple_of(cb * tile, tile), tile)]

    def own_local(cb, a):
        return pltpu.make_async_copy(own_piece(a, cb), out_piece(a, cb, h, core), gl_s.at[cb, a])

    def z_gather(a, cb, o, s, r, to, src=None):
        src = out_piece(a, cb, o, core) if src is None else src
        return remote(src, out_piece(a, cb, o, core), s, r, to)

    def own_sends(cb):
        found = []
        for a in (0, 1):
            found.append(z_gather(a, cb, h, gz_s.at[cb, a, 0], gz_r.at[cb, a, 0], R, own_piece(a, cb)))
            found.append(z_gather(a, cb, h, gz_s.at[cb, a, 1], gz_r.at[cb, a, 1], L, own_piece(a, cb)))
            found.append(z_gather(a, cb, h, gs_s.at[cb, a, 0], gs_r.at[cb, a, 0], sib, own_piece(a, cb)))
        return found

    def forwards(cb):
        return [
            z_gather(0, cb, left_h, gf_s.at[cb, 0], gz_r.at[cb, 0, 2], R),
            z_gather(1, cb, right_h, gf_s.at[cb, 1], gz_r.at[cb, 1, 2], L),
        ]

    def sib_sends(cb, a, k):
        o = (left_h, right_h, far_h)[k]
        return z_gather(a, cb, o, gs_s.at[cb, a, 1 + k], gs_r.at[cb, a, 1 + k], sib)

    def z_arrived(cb, a, k):
        o = (left_h, right_h, far_h)[k]
        ref = out_piece(a, cb, o, core)
        pltpu.make_async_copy(ref, ref, gz_r.at[cb, a, k]).wait()

    def update(cb, carry):
        first_m, second_m = reduced(2 * cb), reduced(2 * cb + 1)
        cols = pl.ds(pl.multiple_of(cb * tile, tile), tile)
        m, p = means_ref[mine_at, cols], prec_ref[mine_at, cols]
        weighted = prior_c * m + step_c * first_m / batch
        new_m = weighted / mass_c
        moved = m - new_m
        spread = (
            prior_c * (1.0 / p + moved * moved)
            + step_c * (second_m - 2.0 * new_m * first_m + new_m * new_m * counts_c) / batch
        )
        stage[0, :, cols] = weighted
        stage[1, :, cols] = spread
        for copy in own_sends(cb):
            copy.start()
        for a in (0, 1):
            own_local(cb, a).start()

        @pl.when(cb > 0)
        def _():
            pass_on(cb - 1)

        return carry

    def pass_on(cb):
        fwd = forwards(cb)
        z_arrived(cb, 0, 0)
        fwd[0].start()
        z_arrived(cb, 1, 1)
        fwd[1].start()
        sib_sends(cb, 0, 0).start()
        sib_sends(cb, 1, 1).start()
        z_arrived(cb, 1, 0)
        sib_sends(cb, 1, 0).start()
        z_arrived(cb, 0, 1)
        sib_sends(cb, 0, 1).start()

    n_cols = width // tile
    lax.fori_loop(0, n_cols, update, 0)
    pass_on(n_cols - 1)

    def finish(cb, carry):
        for a in (0, 1):
            z_arrived(cb, a, 2)
            sib_sends(cb, a, 2).start()
        return carry

    lax.fori_loop(0, n_cols, finish, 0)

    def drain(cb, carry):
        for copy in own_sends(cb) + forwards(cb):
            copy.wait_send()
        for a in (0, 1):
            own_local(cb, a).wait()
            for k in range(3):
                sib_sends(cb, a, k).wait_send()
            for k, o in enumerate((h, left_h, right_h, far_h)):
                ref = out_piece(a, cb, o, 1 - core)
                pltpu.make_async_copy(ref, ref, gs_r.at[cb, a, k]).wait()
        return carry

    lax.fori_loop(0, n_cols, drain, 0)

    def drain_reduce(n, carry):
        sib_copy(n).wait_send()
        for copy in z_copies(n) + acc_copies(n):
            copy.wait_send()
        return carry

    lax.fori_loop(0, n_blocks, drain_reduce, 0)
    for copy in waits + ids_copies + count_copies:
        copy.wait_send()


def local(row_ids, table, means, precisions, mix_logits, step_index):
    comps, width = means.shape
    n_comp, n_dp = lax.axis_size("comp"), lax.axis_size("dp")
    share = table.shape[0] // n_dp
    rows = share * n_comp
    n_ids = row_ids.shape[0]
    tile = 256
    blocks = 2 * width // tile
    n_cols = width // tile
    half = comps // NC
    q = half // NH
    packed = 2 * rows + 256
    anywhere = pl.BlockSpec(memory_space=pl.ANY)
    vmem = pltpu.VMEM
    dma = pltpu.SemaphoreType.DMA
    space = pl.BlockSpec(memory_space=pltpu.VMEM)
    weighted, spread, mass = pl.pallas_call(
        kernel,
        out_shape=(
            jax.ShapeDtypeStruct((comps, width), F32),
            jax.ShapeDtypeStruct((comps, width), F32),
            jax.ShapeDtypeStruct((1, comps), F32),
        ),
        in_specs=[space, anywhere, anywhere, anywhere, space, pl.BlockSpec(memory_space=pltpu.SMEM)],
        out_specs=(anywhere, anywhere, space),
        scratch_shapes=[
            vmem((comps, width), F32),
            vmem((comps, width), F32),
            vmem((2, q, width), F32),
            vmem((n_comp, share, width), F32),
            vmem((n_dp, 1, n_ids), jnp.int32),
            vmem((comps, 2 * width), BF16),
            vmem((comps, 2 * width), BF16),
            vmem((rows, 2 * width), BF16),
            vmem((rows, 2 * width), BF16),
            vmem((comps, rows), F32),
            vmem((comps, rows), BF16),
            vmem((comps, rows), BF16),
            vmem((comps, 1), F32),
            vmem((1, rows), F32),
            vmem((1, rows), F32),
            vmem((comps, 1), F32),
            vmem((NX, 1, packed), F32),
            vmem((NZ * NY, 1, packed), F32),
            vmem((1, rows), F32),
            vmem((1, rows), F32),
            vmem((1, rows), F32),
            vmem((n_dp, 1, comps), F32),
            vmem((comps, 8), F32),
            vmem((blocks, half, tile), F32),
            vmem((blocks, half, tile), F32),
            vmem((blocks, half, tile), F32),
            vmem((blocks, q, tile // 2), F32),
            vmem((blocks, q, tile // 2), F32),
            vmem((blocks, q, tile), F32),
            vmem((blocks, q, tile), F32),
            dma((3,)), dma((n_dp,)), dma((n_dp,)), dma((62,)), dma((n_comp, 2)),
            dma((NX - 1,)), dma((NX,)), dma((NZ * NY - 1,)), dma((NZ * NY,)), dma((n_dp,)), dma((n_dp,)),
            dma((blocks,)), dma((blocks,)), dma((blocks, 2)), dma((blocks, 2)), dma((blocks, 2)),
            dma((blocks, 2)), dma((blocks, 2)), dma((blocks, 2)),
            dma((n_cols, 2, 2)), dma((n_cols, 2, 3)), dma((n_cols, 2)), dma((n_cols, 2, 4)), dma((n_cols, 2, 4)), dma((n_cols, 2)),
        ],
        compiler_params=pltpu.CompilerParams(
            collective_id=0, has_side_effects=True, vmem_limit_bytes=58 * 2**20
        ),
        name="em",
    )(row_ids.reshape(1, n_ids), table, means, precisions, mix_logits.reshape(1, comps), step_index)
    mass = mass.reshape(comps)
    return weighted / mass[:, None], mass[:, None] / spread, jnp.log(mass)


def solution(mesh):
    placed = (P("dp"), P("comp", None), P("comp", None), P("comp", None), P("comp"), P())
    return jax.shard_map(
        local,
        mesh=mesh,
        in_specs=placed,
        out_specs=(P("comp", None), P("comp", None), P("comp")),
        check_vma=False,
    )
```

```python
import functools

import jax
import jax.numpy as jnp
from jax import lax
from jax.experimental import pallas as pl
from jax.experimental.pallas import tpu as pltpu
from jax.sharding import PartitionSpec as P

F32, BF16 = jnp.float32, jnp.bfloat16
NX, NZ, NY = 4, 2, 4
NH, NC = 4, 2
LANES = (((1,), (1,)), ((), ()))
INNER = (((1,), (0,)), ((), ()))


def split(value):
    high = value.astype(BF16)
    return high, (value - high.astype(F32)).astype(BF16)


def mul(left, right, dims, precision=None):
    return lax.dot_general(left, right, dims, precision=precision, preferred_element_type=F32)


class Copy:
    def __init__(self, src, dst, send_sem, recv_sem, to):
        self.make = lambda: pltpu.make_async_remote_copy(
            src_ref=src, dst_ref=dst, send_sem=send_sem, recv_sem=recv_sem, device_id={"dp": to}
        )

    def start(self):
        self.make().start()

    def wait_send(self):
        self.make().wait_send()

    def wait_recv(self):
        self.make().wait_recv()


def kernel(
    ids_ref, table_ref, means_hbm, prec_hbm, logits_ref, step_ref,
    out_m, out_p, out_mass,
    means_ref, prec_ref, stage, rows, ids_all, a_hi, a_lo, f_hi, f_lo, score, r_hi, r_lo, offset, tops, times_ref, counts_col,
    xb, yb, peaks, scale, factors_ref, counts_all, columns,
    sib_out, sib_in, part, from_r, from_l, own_r, own_l,
    local_sem, ids_send, ids_recv, row_send, row_recv, xs, xr, ys, yr, cs, cr,
    sib_s, sib_r, opp_s, opp_r, dir_s, dir_r, acc_s, acc_r,
    gz_s, gz_r, gf_s, gs_s, gs_r, gl_s,
):
    dp, comp = lax.axis_index("dp"), lax.axis_index("comp")
    h, core = lax.div(dp, NC), lax.rem(dp, NC)
    x, zl, y = lax.div(comp, NZ * NY), lax.rem(lax.div(comp, NY), NZ), lax.rem(comp, NY)
    x_at = {d: lax.rem(x + (d % NX), NX) for d in (-1, 0, 1, 2, 3)}
    y_at = {d: lax.rem(y + (d % NY), NY) for d in (-1, 0, 1, 2, 3)}
    z_at = {0: zl, 1: 1 - zl}
    h_at = {d: lax.rem(h + (d % NH), NH) for d in (-1, 0, 1, 2, 3)}
    c_at = {0: core, 1: 1 - core}
    n_dp = NH * NC
    share = rows.shape[1]
    comps, width = means_ref.shape
    n_rows = f_hi.shape[0]

    def at(dx, dz, dy):
        return x_at[dx] * (NZ * NY) + z_at[dz] * NY + y_at[dy]

    def dp_at(dh, dc):
        return h_at[dh] * NC + c_at[dc]

    plane = [(a, b) for a in range(NZ) for b in range(NY) if (a, b) != (0, 0)]
    to_x, to_yz = [at(d, 0, 0) for d in (1, 2, 3)], [at(0, a, b) for a, b in plane]
    peers_c = to_x + to_yz
    peers_d = [dp_at(a, b) for a in range(NH) for b in range(NC) if (a, b) != (0, 0)]
    for k, (src, dst) in enumerate(((means_hbm, means_ref), (prec_hbm, prec_ref))):
        pltpu.make_async_copy(src, dst, local_sem.at[1 + k]).start()
    barrier = pltpu.get_barrier_semaphore()
    for peer in peers_c:
        pl.semaphore_signal(barrier, inc=1, device_id={"comp": peer})
    for peer in peers_d:
        pl.semaphore_signal(barrier, inc=1, device_id={"dp": peer})

    row_block = 32

    def factors(i, carry):
        at_rows = pl.ds(pl.multiple_of(i * row_block, row_block), row_block)
        p, m = prec_ref[at_rows, :], means_ref[at_rows, :]
        cross = p * m
        hi, lo = split(cross)
        a_hi[at_rows, :width], a_lo[at_rows, :width] = hi, lo
        hi, lo = split(-0.5 * (p - 1.0))
        a_hi[at_rows, width:], a_lo[at_rows, width:] = hi, lo
        offset[at_rows, :] = 0.5 * jnp.sum(jnp.log(p) - cross * m, axis=1, keepdims=True)
        return carry

    for k, (src, dst) in enumerate(((means_hbm, means_ref), (prec_hbm, prec_ref))):
        pltpu.make_async_copy(src, dst, local_sem.at[1 + k]).wait()
    lax.fori_loop(0, comps // row_block, factors, 0)
    logits = logits_ref[...]
    turned = jnp.transpose(jnp.broadcast_to(logits, (8, comps)))
    offset[...] = offset[...] + turned[:, 0:1]
    pl.semaphore_wait(barrier, len(peers_c) + len(peers_d))

    waits = []

    def send(src, dst, send_sem, recv_sem, **where):
        copy = pltpu.make_async_remote_copy(
            src_ref=src, dst_ref=dst, send_sem=send_sem, recv_sem=recv_sem, device_id=where
        )
        copy.start()
        return copy

    me = at(0, 0, 0)
    mine = pltpu.make_async_copy(table_ref.at[pl.ds(dp * share, share)], rows.at[me], local_sem.at[0])
    mine.start()
    sends = [0]
    first = [(1, 0, 0), (-1, 0, 0)], [(0, 0, 1), (0, 0, -1)]
    half = share // 2

    def piece(slot, b):
        return rows.at[slot, pl.ds(b * half, half)]

    def push(slot, b, dx, dz, dy, source=None):
        src = piece(slot, b) if source is None else source
        k = sends[0]
        sends[0] += 1
        waits.append(
            send(src, piece(slot, b), row_send.at[k], row_recv.at[slot, b], comp=at(dx, dz, dy))
        )

    def arrived(slot, b):
        pltpu.make_async_copy(piece(slot, b), piece(slot, b), row_recv.at[slot, b]).wait()

    def vec(d, b):
        return (d, 0) if b == 0 else (0, d)

    def own():
        src = [table_ref.at[pl.ds(dp * share + b * half, half)] for b in (0, 1)]
        for b in (0, 1):
            push(me, b, 0, 1, 0, src[b])
        for k in (0, 1):
            for b in (0, 1):
                for to in first[b ^ k]:
                    push(me, b, *to, src[b])

    def partner():
        slot = at(0, 1, 0)
        for b in (0, 1):
            arrived(slot, b)
            for to in first[b] + first[1 - b]:
                push(slot, b, *to)

    def first_near():
        for rel in (0, 1):
            for b in (0, 1):
                for d in (-1, 1):
                    dx, dy = vec(d, b)
                    slot = at(dx, rel, dy)
                    arrived(slot, b)
                    if (rel == 0) == (d == -1):
                        fx, fy = vec(-d, b)
                        push(slot, b, fx, 0, fy)
                    for to in first[1 - b]:
                        push(slot, b, *to)

    def first_far():
        for rel in (0, 1):
            for b in (0, 1):
                dx, dy = vec(2, b)
                slot = at(dx, rel, dy)
                arrived(slot, b)
                for to in first[1 - b]:
                    push(slot, b, *to)

    def second_near(e):
        for rel in (0, 1):
            for b in (0, 1):
                ex, ey = vec(e, b)
                for d in (-1, 1):
                    dx, dy = vec(d, 1 - b)
                    slot = at(ex + dx, rel, ey + dy)
                    arrived(slot, b)
                    if (rel == 0) == (d == -1):
                        fx, fy = vec(-d, 1 - b)
                        push(slot, b, fx, 0, fy)

    def second_far(e):
        for rel in (0, 1):
            for b in (0, 1):
                ex, ey = vec(e, b)
                dx, dy = vec(2, 1 - b)
                arrived(at(ex + dx, rel, ey + dy), b)

    own()
    ids_copies = [
        send(ids_ref, ids_all.at[dp], ids_send.at[k], ids_recv.at[dp], dp=peer)
        for k, peer in enumerate(peers_d)
    ]
    ids_all[dp] = ids_ref[...]

    partner()
    first_near()
    first_far()
    second_near(0)

    owners = NX * NZ * NY
    found = jnp.zeros((owners, share), F32)
    for k, peer in enumerate(peers_d):
        pltpu.make_async_copy(ids_ref, ids_all.at[peer], ids_recv.at[peer]).wait()
    per_owner = n_dp * share
    for k in range(n_dp):
        ids = ids_all[k]
        owner = ids // per_owner
        row = ids - owner * per_owner - dp * share
        left = lax.broadcasted_iota(jnp.int32, (owners, ids.shape[1]), 0) == owner
        right = lax.broadcasted_iota(jnp.int32, (share, ids.shape[1]), 0) == row
        found += mul(left.astype(F32).astype(BF16), right.astype(F32).astype(BF16), LANES)
    flat = lax.broadcasted_iota(jnp.int32, (owners, n_rows), 1)
    slot_of = lax.broadcasted_iota(jnp.int32, (owners, n_rows), 0)
    later = flat - owners * half
    along_x = lax.div(flat, half)
    xz = lax.rem(lax.div(later, half), NX * NZ)
    along_y = xz * NY + lax.div(later, NX * NZ * half)
    pick = (jnp.where(later < 0, along_x, along_y) == slot_of).astype(F32)
    spread_out = mul(found, pick, (((0,), (0,)), ((), ())), lax.Precision.HIGHEST)
    row_of = lax.broadcasted_iota(jnp.int32, (share, n_rows), 0)
    row_flat = lax.broadcasted_iota(jnp.int32, (share, n_rows), 1)
    row_flat = lax.rem(row_flat, half) + jnp.where(row_flat < owners * half, 0, half)
    times_ref[...] = jnp.sum(jnp.where(row_flat == row_of, spread_out, 0.0), axis=0, keepdims=True)

    tile = 256
    block_cols = owners * half // NX
    chunk = 2 * block_cols
    order = (0, -1, 1, 2)

    def places(e):
        return (
            pl.multiple_of(x_at[e] * block_cols, block_cols),
            pl.multiple_of(owners * half + y_at[e] * block_cols, block_cols),
        )

    def features_of(e):
        base = order.index(e) * chunk

        def features(k, carry):
            slots = (x_at[e] * (NZ * NY) + k, k * NY + y_at[e])
            for b in (0, 1):
                s = rows[slots[b], b * half : (b + 1) * half, :]
                here = pl.ds(pl.multiple_of(base + b * block_cols + k * half, half), half)
                f_hi[here, :width], f_lo[here, :width] = split(s)
                f_hi[here, width:], f_lo[here, width:] = split(s * s)
            return carry

        lax.fori_loop(0, NZ * NY, features, 0)

    def scores_of(e):
        base = order.index(e) * chunk
        cols = slice(base, base + chunk)

        def block(k, top):
            here = pl.ds(pl.multiple_of(k * tile, tile), tile)
            fh, fl = f_hi[cols, :], f_lo[cols, :]
            s = mul(a_hi[here, :], fh, LANES) + mul(a_hi[here, :], fl, LANES) + mul(a_lo[here, :], fh, LANES)
            s = s + offset[here, :]
            score[here, cols] = s
            return jnp.maximum(top, jnp.max(s, axis=0, keepdims=True))

        top = lax.fori_loop(0, comps // tile, block, jnp.full((1, chunk), -jnp.inf, F32))

        def raise_block(k, mass):
            here = pl.ds(pl.multiple_of(k * 64, 64), 64)
            e = jnp.exp(score[here, cols] - top)
            score[here, cols] = e
            return mass + jnp.sum(e, axis=0, keepdims=True)

        mass = lax.fori_loop(0, comps // 64, raise_block, jnp.zeros((1, chunk), F32))
        tops[:, cols] = top
        for b, place in enumerate(places(e)):
            part_cols = slice(b * block_cols, (b + 1) * block_cols)
            xb[x, :, pl.ds(place, block_cols)] = top[:, part_cols]
            xb[x, :, pl.ds(pl.multiple_of(n_rows + place, block_cols), block_cols)] = mass[:, part_cols]

    logit_top = jnp.max(logits)
    logit_raised = jnp.exp(logits - logit_top)

    parts = ((0, n_rows, n_rows), (2 * n_rows, 128, 128))

    def combine(ref, n):
        out = []
        for start, size, gap in parts:
            ts = [ref[k, :, start : start + size] for k in range(n)]
            ms = [ref[k, :, start + gap : start + gap + size] for k in range(n)]
            top = functools.reduce(jnp.maximum, ts)
            out.append((start, size, gap, top, sum(m * jnp.exp(a - top) for m, a in zip(ms, ts))))
        return out

    def fill(ref, index, results):
        for start, size, gap, top, m in results:
            ref[index, :, start : start + size] = top
            ref[index, :, start + gap : start + gap + size] = m

    from_x = [x_at[d] for d in (1, 2, 3)]
    from_yz = [z_at[a] * NY + y_at[b] for a, b in plane]
    stages = ((x, to_x, from_x, xs, xr), (zl * NY + y, to_yz, from_yz, ys, yr))

    packs = (xb, yb)

    def stage_send(d):
        ref, (index, to, _, s_sem, r_sem) = packs[d], stages[d]
        for k, peer in enumerate(to):
            waits.append(send(ref.at[index], ref.at[index], s_sem.at[k], r_sem.at[index], comp=peer))

    def stage_wait(d):
        ref, (_, _, slots, _, r_sem) = packs[d], stages[d]
        for slot in slots:
            pltpu.make_async_copy(ref.at[slot], ref.at[slot], r_sem.at[slot]).wait()
        return combine(ref, (NX, NZ * NY)[d])

    xb[x, :, 2 * n_rows : 2 * n_rows + 128] = jnp.full((1, 128), logit_top, F32)
    xb[x, :, 2 * n_rows + 128 :] = jnp.full((1, 128), jnp.sum(logit_raised), F32)
    second_near(-1)
    second_near(1)
    mine.wait()
    second_far(0)
    features_of(0)
    scores_of(0)
    second_near(2)
    second_far(-1)
    features_of(-1)
    scores_of(-1)
    second_far(1)
    features_of(1)
    scores_of(1)
    second_far(2)
    features_of(2)
    scores_of(2)

    stage_send(0)
    fill(yb, stages[1][0], stage_wait(0))
    stage_send(1)
    (_, _, _, peak, total), (_, _, _, logit_peak, logit_total) = stage_wait(1)

    peaks[...] = peak
    scale[...] = times_ref[...] / total
    for k, e in enumerate(order):
        for b, place in enumerate(places(e)):
            cols = slice(k * chunk + b * block_cols, k * chunk + (b + 1) * block_cols)
            at_place = pl.ds(place, block_cols)
            factors_ref[:, cols] = jnp.exp(tops[:, cols] - peaks[:, at_place]) * scale[:, at_place]
    factor = factors_ref[...]

    def responsibilities(which):
        def one(k, carry):
            here = pl.ds(pl.multiple_of(which * (comps // NC) + k * row_block, row_block), row_block)
            r = score[here, :] * factor
            r_hi[here, :], r_lo[here, :] = split(r)
            counts_col[here, :] = jnp.sum(r, axis=1, keepdims=True)
            return carry

        lax.fori_loop(0, comps // NC // row_block, one, 0)

    n_blocks = 2 * width // tile
    own_half = comps // NC
    q = own_half // NH
    side = tile // 2
    L, R = dp_at(-1, 0), dp_at(1, 0)
    sib = dp_at(0, 1)

    def moment(n, which):
        start = pl.multiple_of(lax.rem(n, 2) * width + lax.div(n, 2) * tile, tile)
        cols = pl.ds(start, tile)
        here = pl.ds(pl.multiple_of(which * own_half, own_half), own_half)
        fh, fl, rh = f_hi[:, cols], f_lo[:, cols], r_hi[here, :]
        return mul(rh, fh, INNER) + mul(rh, fl, INNER) + mul(r_lo[here, :], fh, INNER)

    def sib_copy(n):
        return Copy(sib_out.at[n], sib_in.at[n], sib_s.at[n], sib_r.at[n], sib)

    def for_sibling(n):
        sib_out[n] = moment(n, 1 - core)
        sib_copy(n).start()

    def chunk_of(n, o, b):
        return part.at[n, pl.ds(pl.multiple_of(o * q, q), q), pl.ds(b * side, side)]

    left_h, right_h, far_h = h_at[-1], h_at[1], h_at[2]

    def remote(src, dst, s, r, to):
        return Copy(src, dst, s, r, to)

    def cols_of(b):
        return pl.ds(b * side, side)

    def z_copies(n):
        return [
            remote(chunk_of(n, far_h, 0), from_r.at[n], opp_s.at[n, 0], opp_r.at[n, 0], L),
            remote(chunk_of(n, far_h, 1), from_l.at[n], opp_s.at[n, 1], opp_r.at[n, 1], R),
            remote(chunk_of(n, left_h, 1), own_r.at[n, :, cols_of(1)], dir_s.at[n, 0], dir_r.at[n, 0], L),
            remote(chunk_of(n, right_h, 0), own_l.at[n, :, cols_of(0)], dir_s.at[n, 1], dir_r.at[n, 1], R),
        ]

    def acc_copies(n):
        return [
            remote(chunk_of(n, left_h, 0), own_r.at[n, :, cols_of(0)], acc_s.at[n, 0], acc_r.at[n, 0], L),
            remote(chunk_of(n, right_h, 1), own_l.at[n, :, cols_of(1)], acc_s.at[n, 1], acc_r.at[n, 1], R),
        ]

    def relay(n):
        opp, acc = z_copies(n)[:2], acc_copies(n)
        opp[0].wait_recv()
        spot = chunk_of(n, left_h, 0)
        spot[...] = spot[...] + from_r[n]
        acc[0].start()
        opp[1].wait_recv()
        spot = chunk_of(n, right_h, 1)
        spot[...] = spot[...] + from_l[n]
        acc[1].start()

    responsibilities(1 - core)
    for_sibling(0)
    responsibilities(core)

    def reduce_step(n, carry):
        own_block = moment(n, core)
        sib_copy(n).wait_recv()
        part[n] = own_block + sib_in[n]
        for copy in z_copies(n):
            copy.start()

        @pl.when(n + 1 < n_blocks)
        def _():
            for_sibling(n + 1)

        @pl.when(n > 0)
        def _():
            relay(n - 1)

        return carry

    lax.fori_loop(0, 2, reduce_step, 0)
    counts_all[dp] = jnp.transpose(jnp.broadcast_to(counts_col[...], (comps, 8)))[0:1, :]
    count_copies = [
        send(counts_all.at[dp], counts_all.at[dp], cs.at[k], cr.at[dp], dp=peer)
        for k, peer in enumerate(peers_d)
    ]
    lax.fori_loop(2, n_blocks, reduce_step, 0)
    relay(n_blocks - 1)

    for k, peer in enumerate(peers_d):
        pltpu.make_async_copy(counts_all.at[peer], counts_all.at[peer], cr.at[peer]).wait()
    counts = sum(counts_all[k] for k in range(n_dp))
    batch = 1.0 * n_dp * ids_ref.shape[1]
    index = jnp.full((1, comps), step_ref[0].astype(F32), F32)
    step = jnp.exp(-0.6 * jnp.log(2.0 + index / 8192.0))
    retain = 1.0 - step
    weights = logit_raised * (jnp.exp(logit_top - logit_peak[:, 0:1]) / logit_total[:, 0:1])
    prior = retain * weights
    mass_new = prior + step * counts / batch
    out_mass[...] = mass_new
    stacked = jnp.concatenate([mass_new, prior, counts, step, mass_new, prior, counts, step], axis=0)
    columns[...] = jnp.transpose(stacked)

    mine_at = pl.ds(pl.multiple_of(core * own_half + h * q, q), q)
    col = columns[mine_at, :]
    mass_c, prior_c, counts_c, step_c = (col[:, k : k + 1] for k in range(4))

    def reduced(n):
        z, acc = z_copies(n), acc_copies(n)
        for copy in (z[2], z[3], acc[0], acc[1]):
            copy.wait_recv()
        return part[n, pl.ds(pl.multiple_of(h * q, q), q), :] + own_r[n] + own_l[n]

    outs = (out_m, out_p)

    def out_piece(a, cb, o, c):
        here = pl.ds(pl.multiple_of(c * own_half + o * q, q), q)
        return outs[a].at[here, pl.ds(pl.multiple_of(cb * tile, tile), tile)]

    def own_piece(a, cb):
        return stage.at[a, :, pl.ds(pl.multiple_of(cb * tile, tile), tile)]

    def own_local(cb, a):
        return pltpu.make_async_copy(own_piece(a, cb), out_piece(a, cb, h, core), gl_s.at[cb, a])

    def z_gather(a, cb, o, s, r, to, src=None):
        src = out_piece(a, cb, o, core) if src is None else src
        return remote(src, out_piece(a, cb, o, core), s, r, to)

    def own_sends(cb):
        found = []
        for a in (0, 1):
            found.append(z_gather(a, cb, h, gz_s.at[cb, a, 0], gz_r.at[cb, a, 0], R, own_piece(a, cb)))
            found.append(z_gather(a, cb, h, gz_s.at[cb, a, 1], gz_r.at[cb, a, 1], L, own_piece(a, cb)))
            found.append(z_gather(a, cb, h, gs_s.at[cb, a, 0], gs_r.at[cb, a, 0], sib, own_piece(a, cb)))
        return found

    def forwards(cb):
        return [
            z_gather(0, cb, left_h, gf_s.at[cb, 0], gz_r.at[cb, 0, 2], R),
            z_gather(1, cb, right_h, gf_s.at[cb, 1], gz_r.at[cb, 1, 2], L),
        ]

    def sib_sends(cb, a, k):
        o = (left_h, right_h, far_h)[k]
        return z_gather(a, cb, o, gs_s.at[cb, a, 1 + k], gs_r.at[cb, a, 1 + k], sib)

    def z_arrived(cb, a, k):
        o = (left_h, right_h, far_h)[k]
        ref = out_piece(a, cb, o, core)
        pltpu.make_async_copy(ref, ref, gz_r.at[cb, a, k]).wait()

    def update(cb, carry):
        first_m, second_m = reduced(2 * cb), reduced(2 * cb + 1)
        cols = pl.ds(pl.multiple_of(cb * tile, tile), tile)
        m, p = means_ref[mine_at, cols], prec_ref[mine_at, cols]
        weighted = prior_c * m + step_c * first_m / batch
        new_m = weighted / mass_c
        moved = m - new_m
        spread = (
            prior_c * (1.0 / p + moved * moved)
            + step_c * (second_m - 2.0 * new_m * first_m + new_m * new_m * counts_c) / batch
        )
        stage[0, :, cols] = weighted
        stage[1, :, cols] = spread
        for copy in own_sends(cb):
            copy.start()
        for a in (0, 1):
            own_local(cb, a).start()

        @pl.when(cb > 0)
        def _():
            pass_on(cb - 1)

        return carry

    def pass_on(cb):
        fwd = forwards(cb)
        z_arrived(cb, 0, 0)
        fwd[0].start()
        z_arrived(cb, 1, 1)
        fwd[1].start()
        sib_sends(cb, 0, 0).start()
        sib_sends(cb, 1, 1).start()
        z_arrived(cb, 1, 0)
        sib_sends(cb, 1, 0).start()
        z_arrived(cb, 0, 1)
        sib_sends(cb, 0, 1).start()

    n_cols = width // tile
    lax.fori_loop(0, n_cols, update, 0)
    pass_on(n_cols - 1)

    def finish(cb, carry):
        for a in (0, 1):
            z_arrived(cb, a, 2)
            sib_sends(cb, a, 2).start()
        return carry

    lax.fori_loop(0, n_cols, finish, 0)

    def drain(cb, carry):
        for copy in own_sends(cb) + forwards(cb):
            copy.wait_send()
        for a in (0, 1):
            own_local(cb, a).wait()
            for k in range(3):
                sib_sends(cb, a, k).wait_send()
            for k, o in enumerate((h, left_h, right_h, far_h)):
                ref = out_piece(a, cb, o, 1 - core)
                pltpu.make_async_copy(ref, ref, gs_r.at[cb, a, k]).wait()
        return carry

    lax.fori_loop(0, n_cols, drain, 0)

    def drain_reduce(n, carry):
        sib_copy(n).wait_send()
        for copy in z_copies(n) + acc_copies(n):
            copy.wait_send()
        return carry

    lax.fori_loop(0, n_blocks, drain_reduce, 0)
    for copy in waits + ids_copies + count_copies:
        copy.wait_send()


def finish_kernel(weighted_ref, spread_ref, mass_ref, means_out, precisions_out, logits_out):
    mass = mass_ref[...]
    column = jnp.transpose(jnp.broadcast_to(mass, (8, mass.shape[1])))[:, 0:1]
    means_out[...] = weighted_ref[...] / column
    precisions_out[...] = column / spread_ref[...]
    logits_out[...] = jnp.log(mass)


def local(row_ids, table, means, precisions, mix_logits, step_index):
    comps, width = means.shape
    n_comp, n_dp = lax.axis_size("comp"), lax.axis_size("dp")
    share = table.shape[0] // n_dp
    rows = share * n_comp
    n_ids = row_ids.shape[0]
    tile = 256
    blocks = 2 * width // tile
    n_cols = width // tile
    half = comps // NC
    q = half // NH
    packed = 2 * rows + 256
    anywhere = pl.BlockSpec(memory_space=pl.ANY)
    vmem = pltpu.VMEM
    dma = pltpu.SemaphoreType.DMA
    space = pl.BlockSpec(memory_space=pltpu.VMEM)
    weighted, spread, mass = pl.pallas_call(
        kernel,
        out_shape=(
            jax.ShapeDtypeStruct((comps, width), F32),
            jax.ShapeDtypeStruct((comps, width), F32),
            jax.ShapeDtypeStruct((1, comps), F32),
        ),
        in_specs=[space, anywhere, anywhere, anywhere, space, pl.BlockSpec(memory_space=pltpu.SMEM)],
        out_specs=(anywhere, anywhere, space),
        scratch_shapes=[
            vmem((comps, width), F32),
            vmem((comps, width), F32),
            vmem((2, q, width), F32),
            vmem((n_comp, share, width), F32),
            vmem((n_dp, 1, n_ids), jnp.int32),
            vmem((comps, 2 * width), BF16),
            vmem((comps, 2 * width), BF16),
            vmem((rows, 2 * width), BF16),
            vmem((rows, 2 * width), BF16),
            vmem((comps, rows), F32),
            vmem((comps, rows), BF16),
            vmem((comps, rows), BF16),
            vmem((comps, 1), F32),
            vmem((1, rows), F32),
            vmem((1, rows), F32),
            vmem((comps, 1), F32),
            vmem((NX, 1, packed), F32),
            vmem((NZ * NY, 1, packed), F32),
            vmem((1, rows), F32),
            vmem((1, rows), F32),
            vmem((1, rows), F32),
            vmem((n_dp, 1, comps), F32),
            vmem((comps, 8), F32),
            vmem((blocks, half, tile), F32),
            vmem((blocks, half, tile), F32),
            vmem((blocks, half, tile), F32),
            vmem((blocks, q, tile // 2), F32),
            vmem((blocks, q, tile // 2), F32),
            vmem((blocks, q, tile), F32),
            vmem((blocks, q, tile), F32),
            dma((3,)), dma((n_dp,)), dma((n_dp,)), dma((62,)), dma((n_comp, 2)),
            dma((NX - 1,)), dma((NX,)), dma((NZ * NY - 1,)), dma((NZ * NY,)), dma((n_dp,)), dma((n_dp,)),
            dma((blocks,)), dma((blocks,)), dma((blocks, 2)), dma((blocks, 2)), dma((blocks, 2)),
            dma((blocks, 2)), dma((blocks, 2)), dma((blocks, 2)),
            dma((n_cols, 2, 2)), dma((n_cols, 2, 3)), dma((n_cols, 2)), dma((n_cols, 2, 4)), dma((n_cols, 2, 4)), dma((n_cols, 2)),
        ],
        compiler_params=pltpu.CompilerParams(
            collective_id=0, has_side_effects=True, vmem_limit_bytes=58 * 2**20
        ),
        name="em",
    )(row_ids.reshape(1, n_ids), table, means, precisions, mix_logits.reshape(1, comps), step_index)
    rows_at_once = 128
    wide = pl.BlockSpec((rows_at_once, width), lambda i: (i, 0))
    thin = pl.BlockSpec((1, rows_at_once), lambda i: (0, i))
    new_means, new_precisions, new_logits = pl.pallas_call(
        finish_kernel,
        grid=(comps // rows_at_once,),
        out_shape=(
            jax.ShapeDtypeStruct((comps, width), F32),
            jax.ShapeDtypeStruct((comps, width), F32),
            jax.ShapeDtypeStruct((1, comps), F32),
        ),
        in_specs=[wide, wide, thin],
        out_specs=(wide, wide, thin),
        name="finish",
    )(weighted, spread, mass)
    return new_means, new_precisions, new_logits.reshape(comps)


def solution(mesh):
    placed = (P("dp"), P("comp", None), P("comp", None), P("comp", None), P("comp"), P())
    return jax.shard_map(
        local,
        mesh=mesh,
        in_specs=placed,
        out_specs=(P("comp", None), P("comp", None), P("comp")),
        check_vma=False,
    )
```

```python
import functools

import jax
import jax.numpy as jnp
from jax import lax
from jax.experimental import pallas as pl
from jax.experimental.pallas import tpu as pltpu
from jax.sharding import PartitionSpec as P

F32, BF16 = jnp.float32, jnp.bfloat16
NX, NZ, NY = 4, 2, 4
NH, NC = 4, 2
LANES = (((1,), (1,)), ((), ()))
INNER = (((1,), (0,)), ((), ()))


def split(value):
    high = value.astype(BF16)
    return high, (value - high.astype(F32)).astype(BF16)


def mul(left, right, dims, precision=None):
    return lax.dot_general(left, right, dims, precision=precision, preferred_element_type=F32)


class Copy:
    def __init__(self, src, dst, send_sem, recv_sem, to):
        self.make = lambda: pltpu.make_async_remote_copy(
            src_ref=src, dst_ref=dst, send_sem=send_sem, recv_sem=recv_sem, device_id={"dp": to}
        )

    def start(self):
        self.make().start()

    def wait_send(self):
        self.make().wait_send()

    def wait_recv(self):
        self.make().wait_recv()


def kernel(
    ids_ref, table_ref, means_hbm, prec_hbm, logits_ref, step_ref,
    out_m, out_p, out_mass,
    means_ref, prec_ref, stage, rows, ids_all, a_hi, a_lo, f_hi, f_lo, score, r_hi, r_lo, offset, tops, times_ref, counts_col,
    xb, yb, peaks, scale, factors_ref, counts_all, columns,
    sib_out, sib_in, part, from_r, from_l, own_r, own_l,
    local_sem, ids_send, ids_recv, row_send, row_recv, xs, xr, ys, yr, cs, cr,
    sib_s, sib_r, opp_s, opp_r, dir_s, dir_r, acc_s, acc_r,
    gz_s, gz_r, gf_s, gs_s, gs_r, gl_s,
):
    dp, comp = lax.axis_index("dp"), lax.axis_index("comp")
    h, core = lax.div(dp, NC), lax.rem(dp, NC)
    x, zl, y = lax.div(comp, NZ * NY), lax.rem(lax.div(comp, NY), NZ), lax.rem(comp, NY)
    x_at = {d: lax.rem(x + (d % NX), NX) for d in (-1, 0, 1, 2, 3)}
    y_at = {d: lax.rem(y + (d % NY), NY) for d in (-1, 0, 1, 2, 3)}
    z_at = {0: zl, 1: 1 - zl}
    h_at = {d: lax.rem(h + (d % NH), NH) for d in (-1, 0, 1, 2, 3)}
    c_at = {0: core, 1: 1 - core}
    n_dp = NH * NC
    share = rows.shape[1]
    comps, width = means_ref.shape
    n_rows = f_hi.shape[0]

    def at(dx, dz, dy):
        return x_at[dx] * (NZ * NY) + z_at[dz] * NY + y_at[dy]

    def dp_at(dh, dc):
        return h_at[dh] * NC + c_at[dc]

    plane = [(a, b) for a in range(NZ) for b in range(NY) if (a, b) != (0, 0)]
    to_x, to_yz = [at(d, 0, 0) for d in (1, 2, 3)], [at(0, a, b) for a, b in plane]
    peers_c = to_x + to_yz
    peers_d = [dp_at(a, b) for a in range(NH) for b in range(NC) if (a, b) != (0, 0)]
    for k, (src, dst) in enumerate(((means_hbm, means_ref), (prec_hbm, prec_ref))):
        pltpu.make_async_copy(src, dst, local_sem.at[1 + k]).start()
    barrier = pltpu.get_barrier_semaphore()
    for peer in peers_c:
        pl.semaphore_signal(barrier, inc=1, device_id={"comp": peer})
    for peer in peers_d:
        pl.semaphore_signal(barrier, inc=1, device_id={"dp": peer})

    row_block = 32

    def factors(i, carry):
        at_rows = pl.ds(pl.multiple_of(i * row_block, row_block), row_block)
        p, m = prec_ref[at_rows, :], means_ref[at_rows, :]
        cross = p * m
        hi, lo = split(cross)
        a_hi[at_rows, :width], a_lo[at_rows, :width] = hi, lo
        hi, lo = split(-0.5 * (p - 1.0))
        a_hi[at_rows, width:], a_lo[at_rows, width:] = hi, lo
        offset[at_rows, :] = 0.5 * jnp.sum(jnp.log(p) - cross * m, axis=1, keepdims=True)
        return carry

    for k, (src, dst) in enumerate(((means_hbm, means_ref), (prec_hbm, prec_ref))):
        pltpu.make_async_copy(src, dst, local_sem.at[1 + k]).wait()
    lax.fori_loop(0, comps // row_block, factors, 0)
    logits = logits_ref[...]
    turned = jnp.transpose(jnp.broadcast_to(logits, (8, comps)))
    offset[...] = offset[...] + turned[:, 0:1]
    pl.semaphore_wait(barrier, len(peers_c) + len(peers_d))

    waits = []

    def send(src, dst, send_sem, recv_sem, **where):
        copy = pltpu.make_async_remote_copy(
            src_ref=src, dst_ref=dst, send_sem=send_sem, recv_sem=recv_sem, device_id=where
        )
        copy.start()
        return copy

    me = at(0, 0, 0)
    mine = pltpu.make_async_copy(table_ref.at[pl.ds(dp * share, share)], rows.at[me], local_sem.at[0])
    mine.start()
    sends = [0]
    first = [(1, 0, 0), (-1, 0, 0)], [(0, 0, 1), (0, 0, -1)]
    half = share // 2

    def piece(slot, b):
        return rows.at[slot, pl.ds(b * half, half)]

    def push(slot, b, dx, dz, dy, source=None):
        src = piece(slot, b) if source is None else source
        k = sends[0]
        sends[0] += 1
        waits.append(
            send(src, piece(slot, b), row_send.at[k], row_recv.at[slot, b], comp=at(dx, dz, dy))
        )

    def arrived(slot, b):
        pltpu.make_async_copy(piece(slot, b), piece(slot, b), row_recv.at[slot, b]).wait()

    def vec(d, b):
        return (d, 0) if b == 0 else (0, d)

    def own():
        src = [table_ref.at[pl.ds(dp * share + b * half, half)] for b in (0, 1)]
        for b in (0, 1):
            push(me, b, 0, 1, 0, src[b])
        for k in (0, 1):
            for b in (0, 1):
                for to in first[b ^ k]:
                    push(me, b, *to, src[b])

    def partner():
        slot = at(0, 1, 0)
        for b in (0, 1):
            arrived(slot, b)
            for to in first[b] + first[1 - b]:
                push(slot, b, *to)

    def first_near():
        for rel in (0, 1):
            for b in (0, 1):
                for d in (-1, 1):
                    dx, dy = vec(d, b)
                    slot = at(dx, rel, dy)
                    arrived(slot, b)
                    if (rel == 0) == (d == -1):
                        fx, fy = vec(-d, b)
                        push(slot, b, fx, 0, fy)
                    for to in first[1 - b]:
                        push(slot, b, *to)

    def first_far():
        for rel in (0, 1):
            for b in (0, 1):
                dx, dy = vec(2, b)
                slot = at(dx, rel, dy)
                arrived(slot, b)
                for to in first[1 - b]:
                    push(slot, b, *to)

    def second_near(e):
        for rel in (0, 1):
            for b in (0, 1):
                ex, ey = vec(e, b)
                for d in (-1, 1):
                    dx, dy = vec(d, 1 - b)
                    slot = at(ex + dx, rel, ey + dy)
                    arrived(slot, b)
                    if (rel == 0) == (d == -1):
                        fx, fy = vec(-d, 1 - b)
                        push(slot, b, fx, 0, fy)

    def second_far(e):
        for rel in (0, 1):
            for b in (0, 1):
                ex, ey = vec(e, b)
                dx, dy = vec(2, 1 - b)
                arrived(at(ex + dx, rel, ey + dy), b)

    own()
    ids_copies = [
        send(ids_ref, ids_all.at[dp], ids_send.at[k], ids_recv.at[dp], dp=peer)
        for k, peer in enumerate(peers_d)
    ]
    ids_all[dp] = ids_ref[...]

    partner()
    first_near()
    first_far()
    second_near(0)

    owners = NX * NZ * NY
    found = jnp.zeros((owners, share), F32)
    for k, peer in enumerate(peers_d):
        pltpu.make_async_copy(ids_ref, ids_all.at[peer], ids_recv.at[peer]).wait()
    per_owner = n_dp * share
    for k in range(n_dp):
        ids = ids_all[k]
        owner = ids // per_owner
        row = ids - owner * per_owner - dp * share
        left = lax.broadcasted_iota(jnp.int32, (owners, ids.shape[1]), 0) == owner
        right = lax.broadcasted_iota(jnp.int32, (share, ids.shape[1]), 0) == row
        found += mul(left.astype(F32).astype(BF16), right.astype(F32).astype(BF16), LANES)
    flat = lax.broadcasted_iota(jnp.int32, (owners, n_rows), 1)
    slot_of = lax.broadcasted_iota(jnp.int32, (owners, n_rows), 0)
    later = flat - owners * half
    along_x = lax.div(flat, half)
    xz = lax.rem(lax.div(later, half), NX * NZ)
    along_y = xz * NY + lax.div(later, NX * NZ * half)
    pick = (jnp.where(later < 0, along_x, along_y) == slot_of).astype(F32)
    spread_out = mul(found, pick, (((0,), (0,)), ((), ())), lax.Precision.HIGHEST)
    row_of = lax.broadcasted_iota(jnp.int32, (share, n_rows), 0)
    row_flat = lax.broadcasted_iota(jnp.int32, (share, n_rows), 1)
    row_flat = lax.rem(row_flat, half) + jnp.where(row_flat < owners * half, 0, half)
    times_ref[...] = jnp.sum(jnp.where(row_flat == row_of, spread_out, 0.0), axis=0, keepdims=True)

    tile = 256
    block_cols = owners * half // NX
    chunk = 2 * block_cols
    order = (0, -1, 1, 2)

    def places(e):
        return (
            pl.multiple_of(x_at[e] * block_cols, block_cols),
            pl.multiple_of(owners * half + y_at[e] * block_cols, block_cols),
        )

    def features_of(e):
        base = order.index(e) * chunk

        def features(k, carry):
            slots = (x_at[e] * (NZ * NY) + k, k * NY + y_at[e])
            for b in (0, 1):
                s = rows[slots[b], b * half : (b + 1) * half, :]
                here = pl.ds(pl.multiple_of(base + b * block_cols + k * half, half), half)
                f_hi[here, :width], f_lo[here, :width] = split(s)
                f_hi[here, width:], f_lo[here, width:] = split(s * s)
            return carry

        lax.fori_loop(0, NZ * NY, features, 0)

    def scores_of(e):
        base = order.index(e) * chunk
        cols = slice(base, base + chunk)

        def block(k, top):
            here = pl.ds(pl.multiple_of(k * tile, tile), tile)
            fh, fl = f_hi[cols, :], f_lo[cols, :]
            s = mul(a_hi[here, :], fh, LANES) + mul(a_hi[here, :], fl, LANES) + mul(a_lo[here, :], fh, LANES)
            s = s + offset[here, :]
            score[here, cols] = s
            return jnp.maximum(top, jnp.max(s, axis=0, keepdims=True))

        top = lax.fori_loop(0, comps // tile, block, jnp.full((1, chunk), -jnp.inf, F32))

        def raise_block(k, mass):
            here = pl.ds(pl.multiple_of(k * 64, 64), 64)
            e = jnp.exp(score[here, cols] - top)
            score[here, cols] = e
            return mass + jnp.sum(e, axis=0, keepdims=True)

        mass = lax.fori_loop(0, comps // 64, raise_block, jnp.zeros((1, chunk), F32))
        tops[:, cols] = top
        for b, place in enumerate(places(e)):
            part_cols = slice(b * block_cols, (b + 1) * block_cols)
            xb[x, :, pl.ds(place, block_cols)] = top[:, part_cols]
            xb[x, :, pl.ds(pl.multiple_of(n_rows + place, block_cols), block_cols)] = mass[:, part_cols]

    logit_top = jnp.max(logits)
    logit_raised = jnp.exp(logits - logit_top)

    parts = ((0, n_rows, n_rows), (2 * n_rows, 128, 128))

    def combine(ref, n):
        out = []
        for start, size, gap in parts:
            ts = [ref[k, :, start : start + size] for k in range(n)]
            ms = [ref[k, :, start + gap : start + gap + size] for k in range(n)]
            top = functools.reduce(jnp.maximum, ts)
            out.append((start, size, gap, top, sum(m * jnp.exp(a - top) for m, a in zip(ms, ts))))
        return out

    def fill(ref, index, results):
        for start, size, gap, top, m in results:
            ref[index, :, start : start + size] = top
            ref[index, :, start + gap : start + gap + size] = m

    from_x = [x_at[d] for d in (1, 2, 3)]
    from_yz = [z_at[a] * NY + y_at[b] for a, b in plane]
    stages = ((x, to_x, from_x, xs, xr), (zl * NY + y, to_yz, from_yz, ys, yr))

    packs = (xb, yb)

    def stage_send(d):
        ref, (index, to, _, s_sem, r_sem) = packs[d], stages[d]
        for k, peer in enumerate(to):
            waits.append(send(ref.at[index], ref.at[index], s_sem.at[k], r_sem.at[index], comp=peer))

    def stage_wait(d):
        ref, (_, _, slots, _, r_sem) = packs[d], stages[d]
        for slot in slots:
            pltpu.make_async_copy(ref.at[slot], ref.at[slot], r_sem.at[slot]).wait()
        return combine(ref, (NX, NZ * NY)[d])

    xb[x, :, 2 * n_rows : 2 * n_rows + 128] = jnp.full((1, 128), logit_top, F32)
    xb[x, :, 2 * n_rows + 128 :] = jnp.full((1, 128), jnp.sum(logit_raised), F32)
    second_near(-1)
    second_near(1)
    mine.wait()
    second_far(0)
    features_of(0)
    scores_of(0)
    second_near(2)
    second_far(-1)
    features_of(-1)
    scores_of(-1)
    second_far(1)
    features_of(1)
    scores_of(1)
    second_far(2)
    features_of(2)
    scores_of(2)

    stage_send(0)
    fill(yb, stages[1][0], stage_wait(0))
    stage_send(1)
    (_, _, _, peak, total), (_, _, _, logit_peak, logit_total) = stage_wait(1)

    peaks[...] = peak
    scale[...] = times_ref[...] / total
    for k, e in enumerate(order):
        for b, place in enumerate(places(e)):
            cols = slice(k * chunk + b * block_cols, k * chunk + (b + 1) * block_cols)
            at_place = pl.ds(place, block_cols)
            factors_ref[:, cols] = jnp.exp(tops[:, cols] - peaks[:, at_place]) * scale[:, at_place]
    factor = factors_ref[...]

    def responsibilities(which):
        def one(k, carry):
            here = pl.ds(pl.multiple_of(which * (comps // NC) + k * row_block, row_block), row_block)
            r = score[here, :] * factor
            r_hi[here, :], r_lo[here, :] = split(r)
            counts_col[here, :] = jnp.sum(r, axis=1, keepdims=True)
            return carry

        lax.fori_loop(0, comps // NC // row_block, one, 0)

    n_blocks = 2 * width // tile
    own_half = comps // NC
    q = own_half // NH
    side = tile // 2
    L, R = dp_at(-1, 0), dp_at(1, 0)
    sib = dp_at(0, 1)

    def moment(n, which):
        start = pl.multiple_of(lax.rem(n, 2) * width + lax.div(n, 2) * tile, tile)
        cols = pl.ds(start, tile)
        here = pl.ds(pl.multiple_of(which * own_half, own_half), own_half)
        fh, fl, rh = f_hi[:, cols], f_lo[:, cols], r_hi[here, :]
        return mul(rh, fh, INNER) + mul(rh, fl, INNER) + mul(r_lo[here, :], fh, INNER)

    def sib_copy(n):
        return Copy(sib_out.at[n], sib_in.at[n], sib_s.at[n], sib_r.at[n], sib)

    def for_sibling(n):
        sib_out[n] = moment(n, 1 - core)
        sib_copy(n).start()

    def chunk_of(n, o, b):
        return part.at[n, pl.ds(pl.multiple_of(o * q, q), q), pl.ds(b * side, side)]

    left_h, right_h, far_h = h_at[-1], h_at[1], h_at[2]

    def remote(src, dst, s, r, to):
        return Copy(src, dst, s, r, to)

    def cols_of(b):
        return pl.ds(b * side, side)

    def z_copies(n):
        return [
            remote(chunk_of(n, far_h, 0), from_r.at[n], opp_s.at[n, 0], opp_r.at[n, 0], L),
            remote(chunk_of(n, far_h, 1), from_l.at[n], opp_s.at[n, 1], opp_r.at[n, 1], R),
            remote(chunk_of(n, left_h, 1), own_r.at[n, :, cols_of(1)], dir_s.at[n, 0], dir_r.at[n, 0], L),
            remote(chunk_of(n, right_h, 0), own_l.at[n, :, cols_of(0)], dir_s.at[n, 1], dir_r.at[n, 1], R),
        ]

    def acc_copies(n):
        return [
            remote(chunk_of(n, left_h, 0), own_r.at[n, :, cols_of(0)], acc_s.at[n, 0], acc_r.at[n, 0], L),
            remote(chunk_of(n, right_h, 1), own_l.at[n, :, cols_of(1)], acc_s.at[n, 1], acc_r.at[n, 1], R),
        ]

    def relay(n):
        opp, acc = z_copies(n)[:2], acc_copies(n)
        opp[0].wait_recv()
        spot = chunk_of(n, left_h, 0)
        spot[...] = spot[...] + from_r[n]
        acc[0].start()
        opp[1].wait_recv()
        spot = chunk_of(n, right_h, 1)
        spot[...] = spot[...] + from_l[n]
        acc[1].start()

    responsibilities(1 - core)
    for_sibling(0)
    responsibilities(core)

    def reduce_step(n, carry):
        own_block = moment(n, core)
        sib_copy(n).wait_recv()
        part[n] = own_block + sib_in[n]
        for copy in z_copies(n):
            copy.start()

        @pl.when(n + 1 < n_blocks)
        def _():
            for_sibling(n + 1)

        @pl.when(n > 0)
        def _():
            relay(n - 1)

        return carry

    lax.fori_loop(0, 2, reduce_step, 0)
    counts_all[dp] = jnp.transpose(jnp.broadcast_to(counts_col[...], (comps, 8)))[0:1, :]
    count_copies = [
        send(counts_all.at[dp], counts_all.at[dp], cs.at[k], cr.at[dp], dp=peer)
        for k, peer in enumerate(peers_d)
    ]
    lax.fori_loop(2, n_blocks, reduce_step, 0)
    relay(n_blocks - 1)

    for k, peer in enumerate(peers_d):
        pltpu.make_async_copy(counts_all.at[peer], counts_all.at[peer], cr.at[peer]).wait()
    counts = sum(counts_all[k] for k in range(n_dp))
    batch = 1.0 * n_dp * ids_ref.shape[1]
    index = jnp.full((1, comps), step_ref[0].astype(F32), F32)
    step = jnp.exp(-0.6 * jnp.log(2.0 + index / 8192.0))
    retain = 1.0 - step
    weights = logit_raised * (jnp.exp(logit_top - logit_peak[:, 0:1]) / logit_total[:, 0:1])
    prior = retain * weights
    mass_new = prior + step * counts / batch
    out_mass[...] = mass_new
    stacked = jnp.concatenate([mass_new, prior, counts, step, mass_new, prior, counts, step], axis=0)
    columns[...] = jnp.transpose(stacked)

    mine_at = pl.ds(pl.multiple_of(core * own_half + h * q, q), q)
    col = columns[mine_at, :]
    mass_c, prior_c, counts_c, step_c = (col[:, k : k + 1] for k in range(4))

    def reduced(n):
        z, acc = z_copies(n), acc_copies(n)
        for copy in (z[2], z[3], acc[0], acc[1]):
            copy.wait_recv()
        return part[n, pl.ds(pl.multiple_of(h * q, q), q), :] + own_r[n] + own_l[n]

    outs = (out_m, out_p)

    def out_piece(a, cb, o, c):
        here = pl.ds(pl.multiple_of(c * own_half + o * q, q), q)
        return outs[a].at[here, pl.ds(pl.multiple_of(cb * tile, tile), tile)]

    def own_piece(a, cb):
        return stage.at[a, :, pl.ds(pl.multiple_of(cb * tile, tile), tile)]

    def own_local(cb, a):
        return pltpu.make_async_copy(own_piece(a, cb), out_piece(a, cb, h, core), gl_s.at[cb, a])

    def z_gather(a, cb, o, s, r, to, src=None):
        src = out_piece(a, cb, o, core) if src is None else src
        return remote(src, out_piece(a, cb, o, core), s, r, to)

    def own_sends(cb):
        found = []
        for a in (0, 1):
            found.append(z_gather(a, cb, h, gz_s.at[cb, a, 0], gz_r.at[cb, a, 0], R, own_piece(a, cb)))
            found.append(z_gather(a, cb, h, gz_s.at[cb, a, 1], gz_r.at[cb, a, 1], L, own_piece(a, cb)))
            found.append(z_gather(a, cb, h, gs_s.at[cb, a, 0], gs_r.at[cb, a, 0], sib, own_piece(a, cb)))
        return found

    def forwards(cb):
        return [
            z_gather(0, cb, left_h, gf_s.at[cb, 0], gz_r.at[cb, 0, 2], R),
            z_gather(1, cb, right_h, gf_s.at[cb, 1], gz_r.at[cb, 1, 2], L),
        ]

    def sib_sends(cb, a, k):
        o = (left_h, right_h, far_h)[k]
        return z_gather(a, cb, o, gs_s.at[cb, a, 1 + k], gs_r.at[cb, a, 1 + k], sib)

    def z_arrived(cb, a, k):
        o = (left_h, right_h, far_h)[k]
        ref = out_piece(a, cb, o, core)
        pltpu.make_async_copy(ref, ref, gz_r.at[cb, a, k]).wait()

    def update(cb, carry):
        first_m, second_m = reduced(2 * cb), reduced(2 * cb + 1)
        cols = pl.ds(pl.multiple_of(cb * tile, tile), tile)
        m, p = means_ref[mine_at, cols], prec_ref[mine_at, cols]
        weighted = prior_c * m + step_c * first_m / batch
        new_m = weighted / mass_c
        moved = m - new_m
        spread = (
            prior_c * (1.0 / p + moved * moved)
            + step_c * (second_m - 2.0 * new_m * first_m + new_m * new_m * counts_c) / batch
        )
        stage[0, :, cols] = weighted
        stage[1, :, cols] = spread
        for copy in own_sends(cb):
            copy.start()
        for a in (0, 1):
            own_local(cb, a).start()

        @pl.when(cb > 0)
        def _():
            pass_on(cb - 1)

        return carry

    def pass_on(cb):
        fwd = forwards(cb)
        z_arrived(cb, 0, 0)
        fwd[0].start()
        z_arrived(cb, 1, 1)
        fwd[1].start()
        sib_sends(cb, 0, 0).start()
        sib_sends(cb, 1, 1).start()
        z_arrived(cb, 1, 0)
        sib_sends(cb, 1, 0).start()
        z_arrived(cb, 0, 1)
        sib_sends(cb, 0, 1).start()

    n_cols = width // tile
    lax.fori_loop(0, n_cols, update, 0)
    pass_on(n_cols - 1)

    def finish(cb, carry):
        for a in (0, 1):
            z_arrived(cb, a, 2)
            sib_sends(cb, a, 2).start()
        return carry

    lax.fori_loop(0, n_cols, finish, 0)

    def drain(cb, carry):
        for copy in own_sends(cb) + forwards(cb):
            copy.wait_send()
        for a in (0, 1):
            own_local(cb, a).wait()
            for k in range(3):
                sib_sends(cb, a, k).wait_send()
            for k, o in enumerate((h, left_h, right_h, far_h)):
                ref = out_piece(a, cb, o, 1 - core)
                pltpu.make_async_copy(ref, ref, gs_r.at[cb, a, k]).wait()
        return carry

    lax.fori_loop(0, n_cols, drain, 0)

    def drain_reduce(n, carry):
        sib_copy(n).wait_send()
        for copy in z_copies(n) + acc_copies(n):
            copy.wait_send()
        return carry

    lax.fori_loop(0, n_blocks, drain_reduce, 0)
    for copy in waits + ids_copies + count_copies:
        copy.wait_send()


def finish_kernel(weighted_ref, spread_ref, mass_ref, means_out, precisions_out, logits_out):
    mass = mass_ref[...]
    column = jnp.transpose(jnp.broadcast_to(mass, (8, mass.shape[1])))[:, 0:1]
    means_out[...] = weighted_ref[...] / column
    precisions_out[...] = column / spread_ref[...]
    logits_out[...] = jnp.log(mass)


def local(row_ids, table, means, precisions, mix_logits, step_index):
    comps, width = means.shape
    n_comp, n_dp = lax.axis_size("comp"), lax.axis_size("dp")
    share = table.shape[0] // n_dp
    rows = share * n_comp
    n_ids = row_ids.shape[0]
    tile = 256
    blocks = 2 * width // tile
    n_cols = width // tile
    half = comps // NC
    q = half // NH
    packed = 2 * rows + 256
    anywhere = pl.BlockSpec(memory_space=pl.ANY)
    vmem = pltpu.VMEM
    dma = pltpu.SemaphoreType.DMA
    space = pl.BlockSpec(memory_space=pltpu.VMEM)
    weighted, spread, mass = pl.pallas_call(
        kernel,
        out_shape=(
            jax.ShapeDtypeStruct((comps, width), F32),
            jax.ShapeDtypeStruct((comps, width), F32),
            jax.ShapeDtypeStruct((1, comps), F32),
        ),
        in_specs=[space, anywhere, anywhere, anywhere, space, pl.BlockSpec(memory_space=pltpu.SMEM)],
        out_specs=(anywhere, anywhere, space),
        scratch_shapes=[
            vmem((comps, width), F32),
            vmem((comps, width), F32),
            vmem((2, q, width), F32),
            vmem((n_comp, share, width), F32),
            vmem((n_dp, 1, n_ids), jnp.int32),
            vmem((comps, 2 * width), BF16),
            vmem((comps, 2 * width), BF16),
            vmem((rows, 2 * width), BF16),
            vmem((rows, 2 * width), BF16),
            vmem((comps, rows), F32),
            vmem((comps, rows), BF16),
            vmem((comps, rows), BF16),
            vmem((comps, 1), F32),
            vmem((1, rows), F32),
            vmem((1, rows), F32),
            vmem((comps, 1), F32),
            vmem((NX, 1, packed), F32),
            vmem((NZ * NY, 1, packed), F32),
            vmem((1, rows), F32),
            vmem((1, rows), F32),
            vmem((1, rows), F32),
            vmem((n_dp, 1, comps), F32),
            vmem((comps, 8), F32),
            vmem((blocks, half, tile), F32),
            vmem((blocks, half, tile), F32),
            vmem((blocks, half, tile), F32),
            vmem((blocks, q, tile // 2), F32),
            vmem((blocks, q, tile // 2), F32),
            vmem((blocks, q, tile), F32),
            vmem((blocks, q, tile), F32),
            dma((3,)), dma((n_dp,)), dma((n_dp,)), dma((62,)), dma((n_comp, 2)),
            dma((NX - 1,)), dma((NX,)), dma((NZ * NY - 1,)), dma((NZ * NY,)), dma((n_dp,)), dma((n_dp,)),
            dma((blocks,)), dma((blocks,)), dma((blocks, 2)), dma((blocks, 2)), dma((blocks, 2)),
            dma((blocks, 2)), dma((blocks, 2)), dma((blocks, 2)),
            dma((n_cols, 2, 2)), dma((n_cols, 2, 3)), dma((n_cols, 2)), dma((n_cols, 2, 4)), dma((n_cols, 2, 4)), dma((n_cols, 2)),
        ],
        compiler_params=pltpu.CompilerParams(
            collective_id=0, has_side_effects=True, vmem_limit_bytes=58 * 2**20
        ),
        name="em",
    )(row_ids.reshape(1, n_ids), table, means, precisions, mix_logits.reshape(1, comps), step_index)
    rows_at_once = 256
    wide = pl.BlockSpec((rows_at_once, width), lambda i: (i, 0))
    thin = pl.BlockSpec((1, rows_at_once), lambda i: (0, i))
    new_means, new_precisions, new_logits = pl.pallas_call(
        finish_kernel,
        grid=(comps // rows_at_once,),
        out_shape=(
            jax.ShapeDtypeStruct((comps, width), F32),
            jax.ShapeDtypeStruct((comps, width), F32),
            jax.ShapeDtypeStruct((1, comps), F32),
        ),
        in_specs=[wide, wide, thin],
        out_specs=(wide, wide, thin),
        name="finish",
    )(weighted, spread, mass)
    return new_means, new_precisions, new_logits.reshape(comps)


def solution(mesh):
    placed = (P("dp"), P("comp", None), P("comp", None), P("comp", None), P("comp"), P())
    return jax.shard_map(
        local,
        mesh=mesh,
        in_specs=placed,
        out_specs=(P("comp", None), P("comp", None), P("comp")),
        check_vma=False,
    )
```
